32 devices in a mesh: blk: 16 (over z, y, core), rows: 2 (over x).
Axes of the slice: x: 2, y: 2, z: 4, core: 2. Of those that a mesh axis runs over, the one named last changes fastest.
Arguments:
- columns: float32 [2048, 1280], P('blk', 'rows'), may hold values from -9 to 9
- right_factor: float32 [2048, 512], P('blk', 'rows'), may hold values from -6 to 6
Outputs:
- new_columns: float32 [2048, 1280], P('blk', 'rows')
- new_factor: float32 [2048, 512], P('blk', 'rows')
The draws below stay inside these ranges and needn't reach their ends.
All inputs are finite; a program needn't handle non-finite values.
Results may differ from the reference program's by a relative error of at most 0.0003.
Values sent between devices are 32-bit elements; how exact they have to be, the bound alone decides.
A program may use at most 64 MiB of HBM per device.

```python
import jax
import jax.numpy as jnp
from jax import lax

BLOCK = 64
STEPS = 6
ORDER = 2048
ROWS = 1280
FACTOR_ROWS = 512
N_BLK = 16


def draw_columns(key, part):
    noise_key, left_key, right_key = jax.random.split(jax.random.fold_in(key, 17), 3)
    noise_part = jax.random.truncated_normal(noise_key, -4.0, 4.0, (ORDER, ROWS), jnp.float32)
    weights = jnp.array([0.2, 0.15, 0.1, 0.07], jnp.float32)
    left_part = jax.random.truncated_normal(left_key, -3.0, 3.0, (ORDER, 4), jnp.float32) * weights
    right_part = jax.random.truncated_normal(right_key, -3.0, 3.0, (4, ROWS), jnp.float32)
    return noise_part + jnp.dot(left_part, right_part, precision=lax.Precision.HIGHEST)


def level_of(key, extent, shards, low, top_value):
    level = 1.0
    for position, shards_of in shards:
        draws = jax.random.uniform(jax.random.fold_in(jax.random.fold_in(key, 6), position), (shards_of,), jnp.float32, low / len(shards), top_value / len(shards))
        level = level * jnp.repeat(jnp.exp(draws), extent[position] // shards_of).reshape((-1,) + (1,) * (len(extent) - 1 - position))
    return level


def normal_values(rng, shape, spread, limit, cuts=(), kind=jnp.bfloat16):
    drawn = spread * jax.random.normal(rng, shape, jnp.float32)
    if cuts:
        drawn = drawn * level_of(rng, shape, cuts, -0.22, 0.18)
    return jnp.clip(drawn, -limit, limit).astype(kind)


def setup_inputs(seed: int = 0) -> dict:
    seeds = jax.random.split(jax.random.key(seed), 3)
    return {
        "columns": draw_columns(jax.random.fold_in(seeds[2], 71), 0),
        "right_factor": normal_values(seeds[1], (ORDER, FACTOR_ROWS), 1.0, 6.0, ((0, 16), (1, 2)), jnp.float32),
    }


HIGHEST_PREC = lax.Precision.HIGHEST

def orth_factor(square):
    lower_factor = jnp.linalg.cholesky(jnp.dot(square.T, square, precision=HIGHEST_PREC))
    return jax.scipy.linalg.solve_triangular(lower_factor, square.T, lower=True).T

def rotation(pair_gram):
    first_turn = orth_factor(pair_gram)
    return orth_factor(jnp.dot(pair_gram, first_turn, precision=HIGHEST_PREC))

def pass_moving(blocks):
    return jnp.concatenate([blocks[:, :BLOCK], jnp.roll(blocks[:, BLOCK:], 1, axis=0)], axis=1)

def reference(columns, right_factor):
    column_pairs = columns.reshape(N_BLK, 2 * BLOCK, ROWS)
    factor_pairs = right_factor.reshape(N_BLK, 2 * BLOCK, FACTOR_ROWS)

    def advance(current, unused):
        column_pairs, factor_pairs = current
        pair_grams = jnp.einsum('pim,pjm->pij', column_pairs, column_pairs, precision=HIGHEST_PREC)
        rotations = jax.vmap(rotation)(pair_grams)
        column_pairs = jnp.einsum('pij,pim->pjm', rotations, column_pairs, precision=HIGHEST_PREC)
        factor_pairs = jnp.einsum('pij,pim->pjm', rotations, factor_pairs, precision=HIGHEST_PREC)
        return ((pass_moving(column_pairs), pass_moving(factor_pairs)), None)
    final_state, unused = lax.scan(advance, (column_pairs, factor_pairs), None, length=STEPS)
    return (final_state[0].reshape(ORDER, ROWS), final_state[1].reshape(ORDER, FACTOR_ROWS))
```

```python
import jax
import jax.numpy as jnp
from jax import lax
from jax.experimental import pallas as pl
from jax.experimental.pallas import tpu as pltpu
from jax.sharding import PartitionSpec as P

STEPS = 6
PANEL = 16
LANES = 128
MESH = pl.DeviceIdType.MESH

HIGHEST_PREC = lax.Precision.HIGHEST


def dot_nn(a, b):
    return lax.dot_general(
        a, b, (((1,), (0,)), ((), ())), precision=HIGHEST_PREC, preferred_element_type=jnp.float32
    )


def dot_nt(a, b):
    return lax.dot_general(
        a, b, (((1,), (1,)), ((), ())), precision=HIGHEST_PREC, preferred_element_type=jnp.float32
    )


def dot_tn(a, b):
    return lax.dot_general(
        a, b, (((0,), (0,)), ((), ())), precision=HIGHEST_PREC, preferred_element_type=jnp.float32
    )


def eliminate(work, midway=None):
    order, width = work.shape
    panels = order // PANEL
    for panel in range(panels):
        if midway is not None and panel == panels // 2 - 1:
            midway()
        low = panel * PANEL
        high = low + PANEL
        end = min(high + PANEL, order)
        rows = work[low:high, :]
        below = work[high:end, :] if end > high else None
        spread = [
            jnp.broadcast_to(rows[:, low + k : low + k + 1], (PANEL, 128)) for k in range(PANEL)
        ]
        spread_below = None
        if below is not None:
            spread_below = [
                jnp.broadcast_to(below[:, low + k : low + k + 1], (end - high, 128))
                for k in range(PANEL)
            ]
        done = []
        for j in range(PANEL):
            scale = lax.rsqrt(spread[j][j : j + 1, :])
            column = spread[j] * scale
            wide = jnp.concatenate([scale] * (width // 128), axis=1)
            pivot_row = rows[j : j + 1, :] * wide
            done.append(pivot_row)
            wide_column = jnp.concatenate([column] * (width // 128), axis=1)
            if j + 1 < PANEL:
                rows = rows - wide_column * pivot_row
            if below is not None:
                column_below = spread_below[j] * scale
                wide_below = jnp.concatenate([column_below] * (width // 128), axis=1)
                below = below - wide_below * pivot_row
            for k in range(j + 1, PANEL):
                head = spread[k][j : j + 1, :] * scale
                spread[k] = spread[k] - column * head
                if below is not None:
                    spread_below[k] = spread_below[k] - column_below * head
        finished = jnp.concatenate(done, axis=0)
        work[low:high, :] = finished
        if below is not None:
            work[high:end, :] = below
        if end < order:
            work[end:, :] = work[end:, :] - dot_tn(finished[:, end:order], finished)


def grid_of(shape):
    return lax.broadcasted_iota(jnp.int32, shape, 0), lax.broadcasted_iota(jnp.int32, shape, 1)


def trace(square):
    down, across = grid_of(square.shape)
    kept = jnp.where(down == across, square, 0.0)
    return jnp.sum(jnp.sum(kept, axis=0, keepdims=True), axis=1, keepdims=True)


def scale_of(total):
    return jnp.broadcast_to(1.0 / (total * total), (8, LANES))


def orthogonal(turn):
    overlap = dot_nt(turn, turn)
    down, across = grid_of(overlap.shape)
    lower = jnp.where(down > across, overlap, 0.0)
    lower = jnp.where(down == across, 0.5 * (overlap - 1.0), lower)
    return turn - dot_nn(lower, turn)


def lanes(chunk):
    return slice(chunk * LANES, (chunk + 1) * LANES)


def cycle_kernel(
    columns, right_factor, new_columns, new_factor, own, near, stay_fac, sent_fac, held_fac, grams,
    near_grams, lows, near_lows, cross, scale, solve, pair_sent, pair_sem, fac_sent, fac_sem, gram_sent,
    gram_sem, low_sent, low_sem, cross_sent, cross_sem,
):
    half = columns.shape[0] // 2
    order = 2 * half
    col_chunks = columns.shape[1] // LANES
    fac_chunks = right_factor.shape[1] // LANES
    ring, peers = lax.axis_size("blk"), lax.axis_size("rows")
    place, row_place = lax.axis_index("blk"), lax.axis_index("rows")
    right, left = lax.rem(place + 1, ring), lax.rem(place + ring - 1, ring)

    barrier = pltpu.get_barrier_semaphore()
    for neighbour in (left, right):
        pl.semaphore_signal(barrier, inc=1, device_id={"blk": neighbour}, device_id_type=MESH)
    for off in range(1, peers):
        peer = lax.rem(row_place + off, peers)
        pl.semaphore_signal(barrier, inc=1, device_id={"rows": peer}, device_id_type=MESH)

    def to_right(source, target, send_sem, recv_sem):
        return pltpu.make_async_remote_copy(
            src_ref=source,
            dst_ref=target,
            send_sem=send_sem,
            recv_sem=recv_sem,
            device_id={"blk": right},
            device_id_type=MESH,
        )

    def pair_copy(step, chunk):
        return to_right(
            own.at[step, chunk], near.at[step, chunk], pair_sent.at[step, chunk], pair_sem.at[step, chunk]
        )

    def fac_copy(step, chunk):
        return to_right(
            sent_fac.at[step, chunk],
            held_fac.at[step + 1, chunk],
            fac_sent.at[step, chunk],
            fac_sem.at[step, chunk],
        )

    def gram_copy(step):
        return to_right(grams.at[step], near_grams.at[step], gram_sent.at[step], gram_sem.at[step])

    def low_copy(step):
        return to_right(lows.at[step], near_lows.at[step], low_sent.at[step], low_sem.at[step])

    def cross_copy(slot, off):
        part = cross.at[slot, row_place]
        return pltpu.make_async_remote_copy(
            src_ref=part,
            dst_ref=part,
            send_sem=cross_sent.at[slot, off - 1],
            recv_sem=cross_sem.at[slot, off - 1],
            device_id={"rows": lax.rem(row_place + off, peers)},
            device_id_type=MESH,
        )

    def cross_sum(slot):
        total = cross[slot, 0]
        for peer in range(1, peers):
            total = total + cross[slot, peer]
        return total

    total = jnp.zeros((order, order), jnp.float32)
    for chunk in range(col_chunks):
        part = columns[:, lanes(chunk)]
        own[0, chunk] = part
        total = total + dot_nt(part, part)
    cross[0, row_place] = total
    for chunk in range(fac_chunks):
        stay_fac[chunk] = right_factor[:half, lanes(chunk)]
        held_fac[0, chunk] = right_factor[half:, lanes(chunk)]
    pl.semaphore_wait(barrier, 2 + peers - 1)
    for off in range(1, peers):
        cross_copy(0, off).start()
    for chunk in range(col_chunks):
        pair_copy(0, chunk).start()
    for off in range(1, peers):
        cross_copy(0, off).wait()
    grams[0] = cross_sum(0)
    scale[...] = scale_of(trace(grams[0]))

    def advance(step, carry):
        gram_copy(step).start()
        g = grams[step]
        square = dot_nn(g, g) * scale[:1, :]
        solve[:, :order] = dot_nn(square, square)
        solve[:, order:] = square

        def products():
            for chunk in range(col_chunks):
                pair_copy(step, chunk).wait_recv()

            @pl.when(step < STEPS - 1)
            def _():
                total = jnp.zeros((order, order), jnp.float32)
                for chunk in range(col_chunks):
                    total = total + dot_nt(own[step, chunk], near[step, chunk])
                cross[step + 1, row_place] = total
                for off in range(1, peers):
                    cross_copy(step + 1, off).start()

        eliminate(solve, products)
        turn = orthogonal(solve[:, order:])
        top, low = turn[:half], turn[half:]
        lows[step] = low
        low_copy(step).start()

        for chunk in range(col_chunks):
            own[step + 1, chunk, :half] = dot_nn(top, own[step, chunk])

        @pl.when(step > 0)
        def _():
            for chunk in range(fac_chunks):
                fac_copy(step - 1, chunk).wait_recv()

        for chunk in range(fac_chunks):
            turned = dot_nn(turn, jnp.concatenate([stay_fac[chunk], held_fac[step, chunk]], axis=0))
            stay_fac[chunk] = turned[:half]
            sent_fac[step, chunk] = turned[half:]
            fac_copy(step, chunk).start()
        gram_copy(step).wait_recv()

        @pl.when(step < STEPS - 1)
        def _():
            scale[...] = scale_of(trace(grams[step]) + trace(near_grams[step]))
            grams[step + 1, :half, :half] = dot_nt(dot_nn(top, grams[step]), top)
            for off in range(1, peers):
                cross_copy(step + 1, off).wait()
            reach = dot_nn(top, cross_sum(step + 1))
            low_copy(step).wait_recv()
            arrived = near_lows[step]
            term = dot_nt(reach, arrived)
            grams[step + 1, :half, half:] = term
            grams[step + 1, half:, :half] = term.T
            grams[step + 1, half:, half:] = dot_nt(dot_nn(arrived, near_grams[step]), arrived)
            for chunk in range(col_chunks):
                own[step + 1, chunk, half:] = dot_nn(arrived, near[step, chunk])
                pair_copy(step + 1, chunk).start()

        for chunk in range(col_chunks):
            pair_copy(step, chunk).wait_send()
        for chunk in range(fac_chunks):
            fac_copy(step, chunk).wait_send()
        gram_copy(step).wait_send()
        low_copy(step).wait_send()
        return carry

    lax.fori_loop(0, STEPS, advance, 0)
    low_copy(STEPS - 1).wait_recv()
    for chunk in range(col_chunks):
        new_columns[:half, lanes(chunk)] = own[STEPS, chunk, :half]
        new_columns[half:, lanes(chunk)] = dot_nn(near_lows[STEPS - 1], near[STEPS - 1, chunk])
    for chunk in range(fac_chunks):
        fac_copy(STEPS - 1, chunk).wait_recv()
        new_factor[:half, lanes(chunk)] = stay_fac[chunk]
        new_factor[half:, lanes(chunk)] = held_fac[STEPS, chunk]


def body(columns, right_factor):
    order = columns.shape[0]
    half = order // 2
    col_chunks = columns.shape[1] // LANES
    fac_chunks = right_factor.shape[1] // LANES
    peers = lax.axis_size("rows")

    def room(*shape):
        return pltpu.VMEM(shape, jnp.float32)

    return pl.pallas_call(
        cycle_kernel,
        out_shape=[jax.ShapeDtypeStruct(a.shape, a.dtype) for a in (columns, right_factor)],
        in_specs=[pl.BlockSpec(memory_space=pltpu.VMEM)] * 2,
        out_specs=[pl.BlockSpec(memory_space=pltpu.VMEM)] * 2,
        scratch_shapes=[
            room(STEPS + 1, col_chunks, order, LANES),
            room(STEPS, col_chunks, order, LANES),
            room(fac_chunks, half, LANES),
            room(STEPS, fac_chunks, half, LANES),
            room(STEPS + 1, fac_chunks, half, LANES),
            room(STEPS, order, order),
            room(STEPS, order, order),
            room(STEPS, half, order),
            room(STEPS, half, order),
            room(STEPS, peers, order, order),
            room(8, LANES),
            room(order, 2 * order),
            pltpu.SemaphoreType.DMA((STEPS, col_chunks)),
            pltpu.SemaphoreType.DMA((STEPS, col_chunks)),
            pltpu.SemaphoreType.DMA((STEPS, fac_chunks)),
            pltpu.SemaphoreType.DMA((STEPS, fac_chunks)),
            pltpu.SemaphoreType.DMA((STEPS,)),
            pltpu.SemaphoreType.DMA((STEPS,)),
            pltpu.SemaphoreType.DMA((STEPS,)),
            pltpu.SemaphoreType.DMA((STEPS,)),
            pltpu.SemaphoreType.DMA((STEPS, peers - 1)),
            pltpu.SemaphoreType.DMA((STEPS, peers - 1)),
        ],
        compiler_params=pltpu.CompilerParams(collective_id=0, has_side_effects=True),
        name="cycle",
    )(columns, right_factor)


def solution(mesh):
    return jax.shard_map(
        body,
        mesh=mesh,
        in_specs=(P("blk", "rows"), P("blk", "rows")),
        out_specs=(P("blk", "rows"), P("blk", "rows")),
        check_vma=False,
    )
```

```python
import jax
import jax.numpy as jnp
from jax import lax
from jax.experimental import pallas as pl
from jax.experimental.pallas import tpu as pltpu
from jax.sharding import PartitionSpec as P

STEPS = 6
PANEL = 16
LANES = 128
MESH = pl.DeviceIdType.MESH

HIGHEST_PREC = lax.Precision.HIGHEST


def dot_nn(a, b):
    return lax.dot_general(
        a, b, (((1,), (0,)), ((), ())), precision=HIGHEST_PREC, preferred_element_type=jnp.float32
    )


def dot_nt(a, b):
    return lax.dot_general(
        a, b, (((1,), (1,)), ((), ())), precision=HIGHEST_PREC, preferred_element_type=jnp.float32
    )


def dot_tn(a, b):
    return lax.dot_general(
        a, b, (((0,), (0,)), ((), ())), precision=HIGHEST_PREC, preferred_element_type=jnp.float32
    )


def split(a):
    high = a.astype(jnp.bfloat16)
    return high, (a - high.astype(jnp.float32)).astype(jnp.bfloat16)


def split_left(a, axis=1):
    high, low = split(a)
    return jnp.concatenate([high, low, high], axis=axis)


def split_right(b, axis=0):
    high, low = split(b)
    return jnp.concatenate([high, high, low], axis=axis)


def mix(turn, block):
    return lax.dot_general(
        split_left(turn), split_right(block), (((1,), (0,)), ((), ())), preferred_element_type=jnp.float32
    )


def cross_of(a, b):
    return lax.dot_general(
        split_left(a), split_right(b, 1), (((1,), (1,)), ((), ())), preferred_element_type=jnp.float32
    )


def eliminate(work, hooks):
    order, width = work.shape
    panels = order // PANEL
    for panel in range(panels):
        if panel in hooks:
            hooks[panel]()
        low = panel * PANEL
        high = low + PANEL
        end = min(high + PANEL, order)
        rows = work[low:high, :]
        below = work[high:end, :] if end > high else None
        spread = [
            jnp.broadcast_to(rows[:, low + k : low + k + 1], (PANEL, 128)) for k in range(PANEL)
        ]
        spread_below = None
        if below is not None:
            spread_below = [
                jnp.broadcast_to(below[:, low + k : low + k + 1], (end - high, 128))
                for k in range(PANEL)
            ]
        done = []
        for j in range(PANEL):
            scale = lax.rsqrt(spread[j][j : j + 1, :])
            column = spread[j] * scale
            wide = jnp.concatenate([scale] * (width // 128), axis=1)
            pivot_row = rows[j : j + 1, :] * wide
            done.append(pivot_row)
            wide_column = jnp.concatenate([column] * (width // 128), axis=1)
            if j + 1 < PANEL:
                rows = rows - wide_column * pivot_row
            if below is not None:
                column_below = spread_below[j] * scale
                wide_below = jnp.concatenate([column_below] * (width // 128), axis=1)
                below = below - wide_below * pivot_row
            for k in range(j + 1, PANEL):
                head = spread[k][j : j + 1, :] * scale
                spread[k] = spread[k] - column * head
                if below is not None:
                    spread_below[k] = spread_below[k] - column_below * head
        finished = jnp.concatenate(done, axis=0)
        work[low:high, :] = finished
        if below is not None:
            work[high:end, :] = below
        if end < order:
            work[end:, :] = work[end:, :] - dot_tn(finished[:, end:order], finished)


def grid_of(shape):
    return lax.broadcasted_iota(jnp.int32, shape, 0), lax.broadcasted_iota(jnp.int32, shape, 1)


def trace(square):
    down, across = grid_of(square.shape)
    kept = jnp.where(down == across, square, 0.0)
    return jnp.sum(jnp.sum(kept, axis=0, keepdims=True), axis=1, keepdims=True)


def scale_of(total):
    return jnp.broadcast_to(1.0 / (total * total), (8, LANES))


def orthogonal(turn):
    overlap = dot_nt(turn, turn)
    down, across = grid_of(overlap.shape)
    lower = jnp.where(down > across, overlap, 0.0)
    lower = jnp.where(down == across, 0.5 * (overlap - 1.0), lower)
    return turn - dot_nn(lower, turn)


def cycle_kernel(
    columns, right_factor, new_columns, new_factor, stay, moving, near_stay, near_moving, stay_fac, sent_fac,
    held_fac, grams, near_grams, turns, near_turns, first, cross, scale, solve, stay_sent,
    stay_sem, moving_sent, moving_sem, fac_sent, fac_sem, gram_sent, gram_sem, low_sent, low_sem, top_sent,
    top_sem, first_sent, first_sem, cross_sent, cross_sem,
):
    half = columns.shape[0] // 2
    order = 2 * half
    upper, lower, beyond = slice(0, half), slice(half, order), slice(order, order + half)
    square = slice(0, order)
    ring, peers = lax.axis_size("blk"), lax.axis_size("rows")
    place, row_place = lax.axis_index("blk"), lax.axis_index("rows")
    right, left = lax.rem(place + 1, ring), lax.rem(place + ring - 1, ring)

    barrier = pltpu.get_barrier_semaphore()
    for neighbour in (left, right):
        pl.semaphore_signal(barrier, inc=1, device_id={"blk": neighbour}, device_id_type=MESH)
    for off in range(1, peers):
        peer = lax.rem(row_place + off, peers)
        pl.semaphore_signal(barrier, inc=1, device_id={"rows": peer}, device_id_type=MESH)

    def to_right(source, target, send_sem, recv_sem):
        return pltpu.make_async_remote_copy(
            src_ref=source,
            dst_ref=target,
            send_sem=send_sem,
            recv_sem=recv_sem,
            device_id={"blk": right},
            device_id_type=MESH,
        )

    def stay_copy():
        return to_right(stay.at[0], near_stay.at[0], stay_sent, stay_sem)

    def moving_copy(step):
        return to_right(
            moving.at[step], near_moving.at[step], moving_sent.at[step], moving_sem.at[step]
        )

    def fac_copy(step):
        return to_right(
            sent_fac.at[step], held_fac.at[step + 1], fac_sent.at[step], fac_sem.at[step]
        )

    def gram_copy(step):
        return to_right(
            grams.at[step, square], near_grams.at[step], gram_sent.at[step], gram_sem.at[step]
        )

    def low_copy(step):
        return to_right(
            turns.at[step, lower], near_turns.at[step, lower], low_sent.at[step], low_sem.at[step]
        )

    def top_copy(step):
        return to_right(
            turns.at[step, upper], near_turns.at[step, upper], top_sent.at[step], top_sem.at[step]
        )

    def to_peer(part, send_sem, recv_sem, off):
        return pltpu.make_async_remote_copy(
            src_ref=part,
            dst_ref=part,
            send_sem=send_sem.at[off - 1],
            recv_sem=recv_sem.at[off - 1],
            device_id={"rows": lax.rem(row_place + off, peers)},
            device_id_type=MESH,
        )

    def first_copy(slot, off):
        return to_peer(first.at[slot, row_place], first_sent.at[slot], first_sem.at[slot], off)

    def cross_copy(step, off):
        return to_peer(cross.at[step, row_place], cross_sent.at[step], cross_sem.at[step], off)

    def peer_sum(parts, slot):
        total = parts[slot, 0]
        for peer in range(1, peers):
            total = total + parts[slot, peer]
        return total

    def own(step):
        return jnp.concatenate([stay[step], moving[step]], axis=0)

    def near(step):
        return jnp.concatenate([near_stay[step], near_moving[step]], axis=0)

    stay[0] = columns[upper, :]
    moving[0] = columns[lower, :]
    stay_fac[...] = right_factor[upper, :]
    held_fac[0] = right_factor[lower, :]
    pl.semaphore_wait(barrier, 2 + peers - 1)
    moving_copy(0).start()
    stay_copy().start()
    pair = columns[...]
    start = cross_of(pair, pair)
    first[0, row_place] = start[upper]
    first[1, row_place] = start[lower]
    for off in range(1, peers):
        for slot in range(2):
            first_copy(slot, off).start()
    for off in range(1, peers):
        for slot in range(2):
            first_copy(slot, off).wait_recv()
    grams[0, upper] = peer_sum(first, 0)
    grams[0, lower] = peer_sum(first, 1)
    scale[...] = scale_of(trace(grams[0, square]))

    def rotation(step, hooks):
        gram = grams[step, square]
        twice = dot_nn(gram, gram) * scale[:1, :]
        solve[:, :order] = dot_nn(twice, twice)
        solve[:, order:] = twice
        eliminate(solve, hooks)
        turns[step] = orthogonal(solve[:, order:])

    def rotate_factor(step):
        turned = mix(turns[step], jnp.concatenate([stay_fac[...], held_fac[step]], axis=0))
        stay_fac[...] = turned[upper]
        sent_fac[step] = turned[lower]

    def advance(step, carry):
        def pass_gram():
            gram_copy(step).start()

        def products():
            moving_copy(step).wait_recv()
            cross[step, row_place] = cross_of(near_moving[step], own(step))
            for off in range(1, peers):
                cross_copy(step, off).start()

            @pl.when(step == 0)
            def _():
                stay_copy().wait_recv()
                first[2, row_place] = cross_of(near_stay[0], own(0))
                for off in range(1, peers):
                    first_copy(2, off).start()

        rotation(step, {1: pass_gram, 7: products})
        low_copy(step).start()
        top_copy(step).start()

        @pl.when(step > 0)
        def _():
            fac_copy(step - 1).wait_recv()

        turn = turns[step]
        top = turn[upper]
        top_wide = jnp.concatenate([top, jnp.zeros_like(top)], axis=0)
        stay[step + 1] = mix(top, own(step))
        rotate_factor(step)
        grams[step + 1, upper] = dot_nt(dot_nn(top, grams[step, square]), top_wide)
        fac_copy(step).start()
        low_copy(step).wait_recv()
        low = near_turns[step, lower]
        moving[step + 1] = mix(low, near(step))
        moving_copy(step + 1).start()
        top_copy(step).wait_recv()
        gram_copy(step).wait_recv()
        arrived = near_turns[step]
        low_wide = jnp.concatenate([jnp.zeros_like(low), low], axis=0)
        near_stay[step + 1] = mix(arrived[upper], near(step))
        reach = dot_nt(near_grams[step], low_wide)
        scale[...] = scale_of(trace(grams[step, square]) + trace(near_grams[step]))

        @pl.when(step == 0)
        def _():
            for off in range(1, peers):
                first_copy(2, off).wait_recv()
            grams[0, beyond] = peer_sum(first, 2)

        for off in range(1, peers):
            cross_copy(step, off).wait_recv()
        whole = jnp.concatenate([grams[step, beyond], peer_sum(cross, step)], axis=0)
        met = dot_nn(arrived, reach + dot_nt(whole, top_wide))
        grams[step + 1, beyond] = met[upper]
        grams[step + 1, lower] = met[lower]
        flipped = met.T
        across = lax.broadcasted_iota(jnp.int32, (half, order), 1)
        grams[step + 1, upper] = jnp.where(across < half, grams[step + 1, upper], flipped[upper])
        return carry

    lax.fori_loop(0, STEPS - 1, advance, 0)
    last = STEPS - 1
    rotation(last, {})
    low_copy(last).start()
    fac_copy(last - 1).wait_recv()
    rotate_factor(last)
    fac_copy(last).start()
    new_columns[upper, :] = mix(turns[last, upper], own(last))
    new_factor[upper, :] = stay_fac[...]
    moving_copy(last).wait_recv()
    low_copy(last).wait_recv()
    new_columns[lower, :] = mix(near_turns[last, lower], near(last))
    fac_copy(last).wait_recv()
    new_factor[lower, :] = held_fac[STEPS]

    stay_copy().wait_send()
    for off in range(1, peers):
        for slot in range(3):
            first_copy(slot, off).wait_send()
    for step in range(STEPS):
        moving_copy(step).wait_send()
        fac_copy(step).wait_send()
        low_copy(step).wait_send()
        if step < last:
            gram_copy(step).wait_send()
            top_copy(step).wait_send()
            for off in range(1, peers):
                cross_copy(step, off).wait_send()


def body(columns, right_factor):
    order, width = columns.shape
    half = order // 2
    fac_width = right_factor.shape[1]
    peers = lax.axis_size("rows")

    def room(*shape):
        return pltpu.VMEM(shape, jnp.float32)

    def flags(*shape):
        return pltpu.SemaphoreType.DMA(shape)

    return pl.pallas_call(
        cycle_kernel,
        out_shape=[jax.ShapeDtypeStruct(a.shape, a.dtype) for a in (columns, right_factor)],
        in_specs=[pl.BlockSpec(memory_space=pltpu.VMEM)] * 2,
        out_specs=[pl.BlockSpec(memory_space=pltpu.VMEM)] * 2,
        scratch_shapes=[
            room(STEPS, half, width),
            room(STEPS, half, width),
            room(STEPS, half, width),
            room(STEPS, half, width),
            room(half, fac_width),
            room(STEPS, half, fac_width),
            room(STEPS + 1, half, fac_width),
            room(STEPS, order + half, order),
            room(STEPS, order, order),
            room(STEPS, order, order),
            room(STEPS, order, order),
            room(3, peers, half, order),
            room(STEPS, peers, half, order),
            room(8, LANES),
            room(order, 2 * order),
            pltpu.SemaphoreType.DMA,
            pltpu.SemaphoreType.DMA,
            flags(STEPS),
            flags(STEPS),
            flags(STEPS),
            flags(STEPS),
            flags(STEPS),
            flags(STEPS),
            flags(STEPS),
            flags(STEPS),
            flags(STEPS),
            flags(STEPS),
            flags(3, peers - 1),
            flags(3, peers - 1),
            flags(STEPS, peers - 1),
            flags(STEPS, peers - 1),
        ],
        compiler_params=pltpu.CompilerParams(collective_id=0, has_side_effects=True),
        name="cycle",
    )(columns, right_factor)


def solution(mesh):
    return jax.shard_map(
        body,
        mesh=mesh,
        in_specs=(P("blk", "rows"), P("blk", "rows")),
        out_specs=(P("blk", "rows"), P("blk", "rows")),
        check_vma=False,
    )
```

```python
import jax
import jax.numpy as jnp
from jax import lax
from jax.experimental import pallas as pl
from jax.experimental.pallas import tpu as pltpu
from jax.sharding import PartitionSpec as P

STEPS = 6
PANEL = 16
MEET = 5
SHARE = 6
LANES = 128
ROWS = 8
MESH = pl.DeviceIdType.MESH

HIGHEST_PREC = lax.Precision.HIGHEST


def dot_nn(a, b):
    return lax.dot_general(
        a, b, (((1,), (0,)), ((), ())), precision=HIGHEST_PREC, preferred_element_type=jnp.float32
    )


def dot_nt(a, b):
    return lax.dot_general(
        a, b, (((1,), (1,)), ((), ())), precision=HIGHEST_PREC, preferred_element_type=jnp.float32
    )


def dot_tn(a, b):
    return lax.dot_general(
        a, b, (((0,), (0,)), ((), ())), precision=HIGHEST_PREC, preferred_element_type=jnp.float32
    )


def split(a):
    high = a.astype(jnp.bfloat16)
    return high, (a - high.astype(jnp.float32)).astype(jnp.bfloat16)


def split_left(a, axis=1):
    high, low = split(a)
    return jnp.concatenate([high, low, high], axis=axis)


def split_right(b, axis=0):
    high, low = split(b)
    return jnp.concatenate([high, high, low], axis=axis)


def mix(turn, block):
    return lax.dot_general(
        split_left(turn), split_right(block), (((1,), (0,)), ((), ())), preferred_element_type=jnp.float32
    )


def cross_of(a, b):
    return lax.dot_general(
        split_left(a), split_right(b, 1), (((1,), (1,)), ((), ())), preferred_element_type=jnp.float32
    )


def spread_row(block, row):
    return jnp.broadcast_to(block[row : row + 1, :], block.shape)


def spread_lane(block, lane):
    return jnp.broadcast_to(block[:, lane : lane + 1], (block.shape[0], LANES))


def tree_sum(terms):
    while len(terms) > 1:
        terms = [sum(terms[i : i + 2][1:], terms[i]) for i in range(0, len(terms), 2)]
    return terms[0]


def eliminate(work, unit, hooks):
    order, width = work.shape
    panels = order // PANEL
    one = unit[...]
    wide_one = jnp.concatenate([one, one], axis=0)
    ahead = work[:PANEL, :]
    tiles = range(width // LANES)
    down = lax.broadcasted_iota(jnp.int32, (ROWS, LANES), 0)

    def part(block, group, t):
        return block[group * ROWS : (group + 1) * ROWS, t * LANES : (t + 1) * LANES]

    for panel in range(panels):
        if panel in hooks:
            hooks[panel]()
        low = panel * PANEL
        high = low + PANEL
        end = min(high + PANEL, order)
        own = ahead
        rows = [[part(own, g, t) for t in tiles] for g in range(2)]
        result = [rows[0][1], rows[1][1]]
        first_heads, second_heads = [], []
        for k in range(ROWS):
            both = spread_lane(own[:, :LANES], low + k) * wide_one
            first_heads.append(both[:ROWS])
            second_heads.append(both[ROWS:])
        for k in range(ROWS, PANEL):
            second_heads.append(spread_lane(rows[1][0], low + k) * one)
        scales = [jnp.zeros((ROWS, LANES), jnp.float32) for g in range(2)]
        pivot = spread_row(first_heads[0], 0)
        for j in range(ROWS):
            root = lax.rsqrt(pivot)
            inverse = root * root
            if j + 1 < ROWS:
                side = spread_row(first_heads[j], j + 1) * root
                pivot = spread_row(first_heads[j + 1], j + 1) - side * side
            else:
                side = spread_row(second_heads[j], 0) * root
                pivot = spread_row(second_heads[j + 1], 0) - side * side
            column = [first_heads[j] * inverse, second_heads[j] * inverse]
            onward = jnp.where(down > j, column[0], 0.0)
            column[0] = jnp.where(down == j, 1.0 - inverse, column[0])
            scales[0] = jnp.where(down == j, root, scales[0])
            front = [spread_row(rows[0][t], j) for t in tiles]
            rows = [[rows[g][t] - column[g] * front[t] for t in tiles] for g in range(2)]
            front = spread_row(result[0], j)
            result = [result[0] - onward * front, result[1] - column[1] * front]
            for k in range(j + 1, ROWS):
                head = spread_row(first_heads[k], j)
                first_heads[k] = first_heads[k] - column[0] * head
                second_heads[k] = second_heads[k] - column[1] * head
            for k in range(ROWS, PANEL):
                head = spread_row(second_heads[j], k - ROWS)
                second_heads[k] = second_heads[k] - column[1] * head
        above = [spread_lane(rows[0][0], low + k) for k in range(ROWS, PANEL)]
        for j in range(ROWS, PANEL):
            row = j - ROWS
            root = lax.rsqrt(pivot)
            inverse = root * root
            if j + 1 < PANEL:
                side = spread_row(second_heads[j], row + 1) * root
                pivot = spread_row(second_heads[j + 1], row + 1) - side * side
            column = second_heads[j] * inverse
            onward = jnp.where(down > row, column, 0.0)
            column = jnp.where(down == row, 1.0 - inverse, column)
            scales[1] = jnp.where(down == row, root, scales[1])
            rows[1] = [rows[1][t] - column * spread_row(rows[1][t], row) for t in tiles]
            result[1] = result[1] - onward * spread_row(result[1], row)
            for k in range(j + 1, PANEL):
                second_heads[k] = second_heads[k] - column * spread_row(second_heads[k], row)
        for g in range(2):
            start = low + g * ROWS
            work[start : start + ROWS, LANES:] = result[g] * scales[g]
        if end == high:
            continue
        fronts = [[spread_row(rows[1][t], k) for t in tiles] for k in range(ROWS)]
        rows[0] = [
            rows[0][t] - tree_sum([above[k] * fronts[k][t] for k in range(ROWS)]) for t in tiles
        ]
        fronts = [[spread_row(rows[0][t], k) for t in tiles] for k in range(ROWS)] + fronts
        below = work[high:end, :]
        heads = [spread_lane(below[:, :LANES], low + k) for k in range(PANEL)]
        ahead = []
        for g in range(2):
            moved = [
                tree_sum([part(heads[k], g, 0) * fronts[k][t] for k in range(PANEL)]) for t in tiles
            ]
            ahead.append(jnp.concatenate([part(below, g, t) - moved[t] for t in tiles], axis=1))
        ahead = jnp.concatenate(ahead, axis=0)
        if end < order:
            solved = jnp.concatenate([jnp.concatenate(rows[g], axis=1) for g in range(2)], axis=0)
            work[end:, :] = work[end:, :] - trailing(work, low, high, end, solved)


def trailing(work, low, high, end, solved):
    order = work.shape[0]
    parts = [jnp.zeros((low, solved.shape[1]), jnp.float32)] if low else []
    parts += [solved, jnp.zeros((order - high, solved.shape[1]), jnp.float32)]
    return dot_nn(work[end:, :order], jnp.concatenate(parts, axis=0))


def grid_of(shape):
    return lax.broadcasted_iota(jnp.int32, shape, 0), lax.broadcasted_iota(jnp.int32, shape, 1)


def trace(square):
    down, across = grid_of(square.shape)
    kept = jnp.where(down == across, square, 0.0)
    return jnp.sum(jnp.sum(kept, axis=0, keepdims=True), axis=1, keepdims=True)


def scale_of(total):
    return jnp.broadcast_to(1.0 / (total * total), (8, LANES))


def orthogonal(turn):
    overlap = dot_nt(turn, turn)
    down, across = grid_of(overlap.shape)
    lower = jnp.where(down > across, overlap, 0.0)
    lower = jnp.where(down == across, 0.5 * (overlap - 1.0), lower)
    return turn - mix(lower, turn)


def cycle_kernel(
    columns, right_factor, new_columns, new_factor, stay, moving, near_stay, near_moving, stay_fac, sent_fac,
    held_fac, grams, near_grams, turns, near_turns, first, cross, reach, reach_across, scale, unit, solve, stay_sent,
    stay_sem, moving_sent, moving_sem, fac_sent, fac_sem, gram_sent, gram_sem, low_sent, low_sem, top_sent,
    top_sem, first_sent, first_sem, cross_sent, cross_sem,
):
    half = columns.shape[0] // 2
    order = 2 * half
    upper, lower, beyond = slice(0, half), slice(half, order), slice(order, order + half)
    square = slice(0, order)
    ring, peers = lax.axis_size("blk"), lax.axis_size("rows")
    place, row_place = lax.axis_index("blk"), lax.axis_index("rows")
    right, left = lax.rem(place + 1, ring), lax.rem(place + ring - 1, ring)

    barrier = pltpu.get_barrier_semaphore()
    for neighbour in (left, right):
        pl.semaphore_signal(barrier, inc=1, device_id={"blk": neighbour}, device_id_type=MESH)
    for off in range(1, peers):
        peer = lax.rem(row_place + off, peers)
        pl.semaphore_signal(barrier, inc=1, device_id={"rows": peer}, device_id_type=MESH)

    def to_right(source, target, send_sem, recv_sem):
        return pltpu.make_async_remote_copy(
            src_ref=source,
            dst_ref=target,
            send_sem=send_sem,
            recv_sem=recv_sem,
            device_id={"blk": right},
            device_id_type=MESH,
        )

    def stay_copy():
        return to_right(stay.at[0], near_stay.at[0], stay_sent, stay_sem)

    def moving_copy(step):
        return to_right(
            moving.at[step], near_moving.at[step], moving_sent.at[step], moving_sem.at[step]
        )

    def fac_copy(step):
        return to_right(
            sent_fac.at[step], held_fac.at[step + 1], fac_sent.at[step], fac_sem.at[step]
        )

    def gram_copy(step):
        return to_right(
            grams.at[step], near_grams.at[step], gram_sent.at[step], gram_sem.at[step]
        )

    def low_copy(step):
        return to_right(
            turns.at[step, lower], near_turns.at[step, lower], low_sent.at[step], low_sem.at[step]
        )

    def top_copy(step):
        return to_right(
            turns.at[step, upper], near_turns.at[step, upper], top_sent.at[step], top_sem.at[step]
        )

    def to_peer(part, send_sem, recv_sem, off):
        return pltpu.make_async_remote_copy(
            src_ref=part,
            dst_ref=part,
            send_sem=send_sem.at[off - 1],
            recv_sem=recv_sem.at[off - 1],
            device_id={"rows": lax.rem(row_place + off, peers)},
            device_id_type=MESH,
        )

    def first_copy(slot, off):
        return to_peer(first.at[slot, row_place], first_sent.at[slot], first_sem.at[slot], off)

    def cross_copy(step, off):
        return to_peer(cross.at[step, row_place], cross_sent.at[step], cross_sem.at[step], off)

    def peer_sum(parts, slot):
        total = parts[slot, 0]
        for peer in range(1, peers):
            total = total + parts[slot, peer]
        return total

    def own(step):
        return jnp.concatenate([stay[step], moving[step]], axis=0)

    def near(step):
        return jnp.concatenate([near_stay[step], near_moving[step]], axis=0)

    unit[...] = jnp.ones_like(unit)
    stay[0] = columns[upper, :]
    moving[0] = columns[lower, :]
    stay_fac[...] = right_factor[upper, :]
    held_fac[0] = right_factor[lower, :]
    pl.semaphore_wait(barrier, 2 + peers - 1)
    moving_copy(0).start()
    stay_copy().start()
    pair = columns[...]
    start = cross_of(pair, pair)
    first[0, row_place] = start[upper]
    first[1, row_place] = start[lower]
    for off in range(1, peers):
        for slot in range(2):
            first_copy(slot, off).start()
    for off in range(1, peers):
        for slot in range(2):
            first_copy(slot, off).wait_recv()
    grams[0, upper] = peer_sum(first, 0)
    grams[0, lower] = peer_sum(first, 1)
    scale[...] = scale_of(trace(grams[0]))

    def rotation(step, hooks):
        gram = grams[step]
        twice = dot_nn(gram, gram) * scale[:1, :]
        solve[:, :order] = dot_nn(twice, twice)
        solve[:, order:] = twice
        eliminate(solve, unit, hooks)
        if order // PANEL in hooks:
            hooks[order // PANEL]()
        turns[step, square] = orthogonal(solve[:, order:])
        low_copy(step).start()

    def rotate_factor(step):
        turned = mix(turns[step, square], jnp.concatenate([stay_fac[...], held_fac[step]], axis=0))
        stay_fac[...] = turned[upper]
        sent_fac[step] = turned[lower]

    def meet(step):
        moving_copy(step).wait_recv()
        cross[step, row_place] = cross_of(near_moving[step], own(step))

    def share(step):
        for off in range(1, peers):
            cross_copy(step, off).start()

    def meet_first():
        meet(0)
        stay_copy().wait_recv()
        first[2, row_place] = cross_of(near_stay[0], own(0))

    def share_first():
        share(0)
        for off in range(1, peers):
            first_copy(2, off).start()

    last = STEPS - 1
    gram_copy(0).start()
    rotation(0, {MEET: meet_first, SHARE: share_first})
    top_copy(0).start()
    for off in range(1, peers):
        first_copy(2, off).wait_recv()
    turns[0, beyond] = peer_sum(first, 2)

    def advance(step, carry):
        then = step + 1
        top = turns[step, upper]
        top_wide = jnp.concatenate([top, jnp.zeros_like(top)], axis=0)
        grams[then, upper] = dot_nt(dot_nn(top, grams[step]), top_wide)
        stay[then] = mix(top, own(step))

        @pl.when(step > 0)
        def _():
            fac_copy(step - 1).wait_recv()

        rotate_factor(step)
        fac_copy(step).start()
        gram_copy(step).wait_recv()
        scale[...] = scale_of(trace(grams[step]) + trace(near_grams[step]))
        for off in range(1, peers):
            cross_copy(step, off).wait_recv()
        whole = jnp.concatenate([turns[step, beyond], peer_sum(cross, step)], axis=0)
        reach[...] = dot_nt(whole, top_wide)
        reach_across[...] = dot_nt(top, whole)
        low_copy(step).wait_recv()
        low = near_turns[step, lower]
        moving[then] = mix(low, near(step))
        moving_copy(then).start()
        low_wide = jnp.concatenate([jnp.zeros_like(low), low], axis=0)
        reach[...] += dot_nt(near_grams[step], low_wide)
        grams[then, upper] += dot_nt(reach_across[...], low_wide)
        grams[then, lower] = dot_nn(low, reach[...])

        @pl.when(then < last)
        def _():
            gram_copy(then).start()

        def share_then():
            @pl.when(then < last)
            def _():
                share(then)

        rotation(then, {MEET: lambda: meet(then), SHARE: share_then})

        @pl.when(then < last)
        def _():
            top_copy(then).start()

        top_copy(step).wait_recv()
        arrived = near_turns[step, upper]
        near_stay[then] = mix(arrived, near(step))
        turns[then, beyond] = dot_nn(arrived, reach[...])
        return carry

    lax.fori_loop(0, last, advance, 0)
    fac_copy(last - 1).wait_recv()
    rotate_factor(last)
    fac_copy(last).start()
    new_columns[upper, :] = mix(turns[last, upper], own(last))
    new_factor[upper, :] = stay_fac[...]
    low_copy(last).wait_recv()
    new_columns[lower, :] = mix(near_turns[last, lower], near(last))
    fac_copy(last).wait_recv()
    new_factor[lower, :] = held_fac[STEPS]

    stay_copy().wait_send()
    for off in range(1, peers):
        for slot in range(3):
            first_copy(slot, off).wait_send()
    for step in range(STEPS):
        moving_copy(step).wait_send()
        fac_copy(step).wait_send()
        low_copy(step).wait_send()
        if step < last:
            gram_copy(step).wait_send()
            top_copy(step).wait_send()
            for off in range(1, peers):
                cross_copy(step, off).wait_send()


def body(columns, right_factor):
    order, width = columns.shape
    half = order // 2
    fac_width = right_factor.shape[1]
    peers = lax.axis_size("rows")

    def room(*shape):
        return pltpu.VMEM(shape, jnp.float32)

    def flags(*shape):
        return pltpu.SemaphoreType.DMA(shape)

    return pl.pallas_call(
        cycle_kernel,
        out_shape=[jax.ShapeDtypeStruct(a.shape, a.dtype) for a in (columns, right_factor)],
        in_specs=[pl.BlockSpec(memory_space=pltpu.VMEM)] * 2,
        out_specs=[pl.BlockSpec(memory_space=pltpu.VMEM)] * 2,
        scratch_shapes=[
            room(STEPS, half, width),
            room(STEPS, half, width),
            room(STEPS, half, width),
            room(STEPS, half, width),
            room(half, fac_width),
            room(STEPS, half, fac_width),
            room(STEPS + 1, half, fac_width),
            room(STEPS, order, order),
            room(STEPS, order, order),
            room(STEPS, order + half, order),
            room(STEPS, order, order),
            room(3, peers, half, order),
            room(STEPS, peers, half, order),
            room(order, order),
            room(half, order),
            room(8, LANES),
            room(8, LANES),
            room(order, 2 * order),
            pltpu.SemaphoreType.DMA,
            pltpu.SemaphoreType.DMA,
            flags(STEPS),
            flags(STEPS),
            flags(STEPS),
            flags(STEPS),
            flags(STEPS),
            flags(STEPS),
            flags(STEPS),
            flags(STEPS),
            flags(STEPS),
            flags(STEPS),
            flags(3, peers - 1),
            flags(3, peers - 1),
            flags(STEPS, peers - 1),
            flags(STEPS, peers - 1),
        ],
        compiler_params=pltpu.CompilerParams(
            collective_id=0, has_side_effects=True, vmem_limit_bytes=24 * 1024 * 1024
        ),
        name="cycle",
    )(columns, right_factor)


def solution(mesh):
    return jax.shard_map(
        body,
        mesh=mesh,
        in_specs=(P("blk", "rows"), P("blk", "rows")),
        out_specs=(P("blk", "rows"), P("blk", "rows")),
        check_vma=False,
    )
```

```python
import jax
import jax.numpy as jnp
from jax import lax
from jax.experimental import pallas as pl
from jax.experimental.pallas import tpu as pltpu
from jax.sharding import PartitionSpec as P

STEPS = 6
PANEL = 16
MEET = 5
SHARE = 6
LANES = 128
ROWS = 8
MESH = pl.DeviceIdType.MESH

HIGHEST_PREC = lax.Precision.HIGHEST


def dot_nn(a, b):
    return lax.dot_general(
        a, b, (((1,), (0,)), ((), ())), precision=HIGHEST_PREC, preferred_element_type=jnp.float32
    )


def dot_nt(a, b):
    return lax.dot_general(
        a, b, (((1,), (1,)), ((), ())), precision=HIGHEST_PREC, preferred_element_type=jnp.float32
    )


def dot_tn(a, b):
    return lax.dot_general(
        a, b, (((0,), (0,)), ((), ())), precision=HIGHEST_PREC, preferred_element_type=jnp.float32
    )


def split(a):
    high = a.astype(jnp.bfloat16)
    return high, (a - high.astype(jnp.float32)).astype(jnp.bfloat16)


def split_left(a, axis=1):
    high, low = split(a)
    return jnp.concatenate([high, low, high], axis=axis)


def split_right(b, axis=0):
    high, low = split(b)
    return jnp.concatenate([high, high, low], axis=axis)


def split_three(a):
    high = a.astype(jnp.bfloat16)
    rest = a - high.astype(jnp.float32)
    mid = rest.astype(jnp.bfloat16)
    return high, mid, (rest - mid.astype(jnp.float32)).astype(jnp.bfloat16)


def six_left(a):
    high, mid, low = split_three(a)
    return jnp.concatenate([low, high, mid, mid, high, high], axis=1)


def six_right(b, axis):
    high, mid, low = split_three(b)
    return jnp.concatenate([high, low, mid, high, mid, high], axis=axis)


def six_nn(a, b):
    return lax.dot_general(
        six_left(a), six_right(b, 0), (((1,), (0,)), ((), ())), preferred_element_type=jnp.float32
    )


def six_nt(a, b):
    return lax.dot_general(
        six_left(a), six_right(b, 1), (((1,), (1,)), ((), ())), preferred_element_type=jnp.float32
    )


def mix(turn, block):
    return lax.dot_general(
        split_left(turn), split_right(block), (((1,), (0,)), ((), ())), preferred_element_type=jnp.float32
    )


def cross_of(a, b):
    return lax.dot_general(
        split_left(a), split_right(b, 1), (((1,), (1,)), ((), ())), preferred_element_type=jnp.float32
    )


def spread_row(block, row):
    return jnp.broadcast_to(block[row : row + 1, :], block.shape)


def spread_lane(block, lane):
    return jnp.broadcast_to(block[:, lane : lane + 1], (block.shape[0], LANES))


def tree_sum(terms):
    while len(terms) > 1:
        terms = [sum(terms[i : i + 2][1:], terms[i]) for i in range(0, len(terms), 2)]
    return terms[0]


def eliminate(work, unit, hooks):
    order, width = work.shape
    panels = order // PANEL
    one = unit[...]
    wide_one = jnp.concatenate([one, one], axis=0)
    ahead = work[:PANEL, :]
    tiles = range(width // LANES)
    down = lax.broadcasted_iota(jnp.int32, (ROWS, LANES), 0)

    def part(block, group, t):
        return block[group * ROWS : (group + 1) * ROWS, t * LANES : (t + 1) * LANES]

    for panel in range(panels):
        if panel in hooks:
            hooks[panel]()
        low = panel * PANEL
        high = low + PANEL
        end = min(high + PANEL, order)
        own = ahead
        rows = [[part(own, g, t) for t in tiles] for g in range(2)]
        result = [rows[0][1], rows[1][1]]
        first_heads, second_heads = [], []
        for k in range(ROWS):
            both = spread_lane(own[:, :LANES], low + k) * wide_one
            first_heads.append(both[:ROWS])
            second_heads.append(both[ROWS:])
        for k in range(ROWS, PANEL):
            second_heads.append(spread_lane(rows[1][0], low + k) * one)
        scales = [jnp.zeros((ROWS, LANES), jnp.float32) for g in range(2)]
        pivot = spread_row(first_heads[0], 0)
        for j in range(ROWS):
            root = lax.rsqrt(pivot)
            inverse = root * root
            if j + 1 < ROWS:
                side = spread_row(first_heads[j], j + 1) * root
                pivot = spread_row(first_heads[j + 1], j + 1) - side * side
            else:
                side = spread_row(second_heads[j], 0) * root
                pivot = spread_row(second_heads[j + 1], 0) - side * side
            column = [first_heads[j] * inverse, second_heads[j] * inverse]
            onward = jnp.where(down > j, column[0], 0.0)
            column[0] = jnp.where(down == j, 1.0 - inverse, column[0])
            scales[0] = jnp.where(down == j, root, scales[0])
            front = [spread_row(rows[0][t], j) for t in tiles]
            rows = [[rows[g][t] - column[g] * front[t] for t in tiles] for g in range(2)]
            front = spread_row(result[0], j)
            result = [result[0] - onward * front, result[1] - column[1] * front]
            for k in range(j + 1, ROWS):
                head = spread_row(first_heads[k], j)
                first_heads[k] = first_heads[k] - column[0] * head
                second_heads[k] = second_heads[k] - column[1] * head
            for k in range(ROWS, PANEL):
                head = spread_row(second_heads[j], k - ROWS)
                second_heads[k] = second_heads[k] - column[1] * head
        above = [spread_lane(rows[0][0], low + k) for k in range(ROWS, PANEL)]
        for j in range(ROWS, PANEL):
            row = j - ROWS
            root = lax.rsqrt(pivot)
            inverse = root * root
            if j + 1 < PANEL:
                side = spread_row(second_heads[j], row + 1) * root
                pivot = spread_row(second_heads[j + 1], row + 1) - side * side
            column = second_heads[j] * inverse
            onward = jnp.where(down > row, column, 0.0)
            column = jnp.where(down == row, 1.0 - inverse, column)
            scales[1] = jnp.where(down == row, root, scales[1])
            rows[1] = [rows[1][t] - column * spread_row(rows[1][t], row) for t in tiles]
            result[1] = result[1] - onward * spread_row(result[1], row)
            for k in range(j + 1, PANEL):
                second_heads[k] = second_heads[k] - column * spread_row(second_heads[k], row)
        for g in range(2):
            start = low + g * ROWS
            work[start : start + ROWS, LANES:] = result[g] * scales[g]
        if end == high:
            continue
        fronts = [[spread_row(rows[1][t], k) for t in tiles] for k in range(ROWS)]
        rows[0] = [
            rows[0][t] - tree_sum([above[k] * fronts[k][t] for k in range(ROWS)]) for t in tiles
        ]
        fronts = [[spread_row(rows[0][t], k) for t in tiles] for k in range(ROWS)] + fronts
        below = work[high:end, :]
        heads = [spread_lane(below[:, :LANES], low + k) for k in range(PANEL)]
        ahead = []
        for g in range(2):
            moved = [
                tree_sum([part(heads[k], g, 0) * fronts[k][t] for k in range(PANEL)]) for t in tiles
            ]
            ahead.append(jnp.concatenate([part(below, g, t) - moved[t] for t in tiles], axis=1))
        ahead = jnp.concatenate(ahead, axis=0)
        if end < order:
            solved = jnp.concatenate([jnp.concatenate(rows[g], axis=1) for g in range(2)], axis=0)
            work[end:, :] = work[end:, :] - trailing(work, low, high, end, solved)


def trailing(work, low, high, end, solved):
    order = work.shape[0]
    parts = [jnp.zeros((low, solved.shape[1]), jnp.float32)] if low else []
    parts += [solved, jnp.zeros((order - high, solved.shape[1]), jnp.float32)]
    return dot_nn(work[end:, :order], jnp.concatenate(parts, axis=0))


def grid_of(shape):
    return lax.broadcasted_iota(jnp.int32, shape, 0), lax.broadcasted_iota(jnp.int32, shape, 1)


def trace(square):
    down, across = grid_of(square.shape)
    kept = jnp.where(down == across, square, 0.0)
    return jnp.sum(jnp.sum(kept, axis=0, keepdims=True), axis=1, keepdims=True)


def scale_of(total):
    return jnp.broadcast_to(1.0 / (total * total), (8, LANES))


def orthogonal(turn):
    overlap = six_nt(turn, turn)
    down, across = grid_of(overlap.shape)
    lower = jnp.where(down > across, overlap, 0.0)
    lower = jnp.where(down == across, 0.5 * (overlap - 1.0), lower)
    return turn - mix(lower, turn)


def cycle_kernel(
    columns, right_factor, new_columns, new_factor, stay, moving, near_stay, near_moving, stay_fac, sent_fac,
    held_fac, grams, near_grams, turns, near_turns, first, cross, reach, reach_across, scale, unit, solve, stay_sent,
    stay_sem, moving_sent, moving_sem, fac_sent, fac_sem, gram_sent, gram_sem, low_sent, low_sem, top_sent,
    top_sem, first_sent, first_sem, cross_sent, cross_sem,
):
    half = columns.shape[0] // 2
    order = 2 * half
    upper, lower, beyond = slice(0, half), slice(half, order), slice(order, order + half)
    square = slice(0, order)
    ring, peers = lax.axis_size("blk"), lax.axis_size("rows")
    place, row_place = lax.axis_index("blk"), lax.axis_index("rows")
    right, left = lax.rem(place + 1, ring), lax.rem(place + ring - 1, ring)

    barrier = pltpu.get_barrier_semaphore()
    for neighbour in (left, right):
        pl.semaphore_signal(barrier, inc=1, device_id={"blk": neighbour}, device_id_type=MESH)
    for off in range(1, peers):
        peer = lax.rem(row_place + off, peers)
        pl.semaphore_signal(barrier, inc=1, device_id={"rows": peer}, device_id_type=MESH)

    def to_right(source, target, send_sem, recv_sem):
        return pltpu.make_async_remote_copy(
            src_ref=source,
            dst_ref=target,
            send_sem=send_sem,
            recv_sem=recv_sem,
            device_id={"blk": right},
            device_id_type=MESH,
        )

    def stay_copy():
        return to_right(stay.at[0], near_stay.at[0], stay_sent, stay_sem)

    def moving_copy(step):
        return to_right(
            moving.at[step], near_moving.at[step], moving_sent.at[step], moving_sem.at[step]
        )

    def fac_copy(step):
        return to_right(
            sent_fac.at[step], held_fac.at[step + 1], fac_sent.at[step], fac_sem.at[step]
        )

    def gram_copy(step):
        return to_right(
            grams.at[step], near_grams.at[step], gram_sent.at[step], gram_sem.at[step]
        )

    def low_copy(step):
        return to_right(
            turns.at[step, lower], near_turns.at[step, lower], low_sent.at[step], low_sem.at[step]
        )

    def top_copy(step):
        return to_right(
            turns.at[step, upper], near_turns.at[step, upper], top_sent.at[step], top_sem.at[step]
        )

    def to_peer(part, send_sem, recv_sem, off):
        return pltpu.make_async_remote_copy(
            src_ref=part,
            dst_ref=part,
            send_sem=send_sem.at[off - 1],
            recv_sem=recv_sem.at[off - 1],
            device_id={"rows": lax.rem(row_place + off, peers)},
            device_id_type=MESH,
        )

    def first_copy(slot, off):
        return to_peer(first.at[slot, row_place], first_sent.at[slot], first_sem.at[slot], off)

    def cross_copy(step, off):
        return to_peer(cross.at[step, row_place], cross_sent.at[step], cross_sem.at[step], off)

    def peer_sum(parts, slot):
        total = parts[slot, 0]
        for peer in range(1, peers):
            total = total + parts[slot, peer]
        return total

    def own(step):
        return jnp.concatenate([stay[step], moving[step]], axis=0)

    def near(step):
        return jnp.concatenate([near_stay[step], near_moving[step]], axis=0)

    unit[...] = jnp.ones_like(unit)
    stay[0] = columns[upper, :]
    moving[0] = columns[lower, :]
    stay_fac[...] = right_factor[upper, :]
    held_fac[0] = right_factor[lower, :]
    pl.semaphore_wait(barrier, 2 + peers - 1)
    moving_copy(0).start()
    stay_copy().start()
    pair = columns[...]
    start = cross_of(pair, pair)
    first[0, row_place] = start[upper]
    first[1, row_place] = start[lower]
    for off in range(1, peers):
        for slot in range(2):
            first_copy(slot, off).start()
    for off in range(1, peers):
        for slot in range(2):
            first_copy(slot, off).wait_recv()
    grams[0, upper] = peer_sum(first, 0)
    grams[0, lower] = peer_sum(first, 1)
    scale[...] = scale_of(trace(grams[0]))

    def rotation(step, hooks):
        gram = grams[step]
        twice = six_nn(gram, gram) * scale[:1, :]
        solve[:, :order] = six_nn(twice, twice)
        solve[:, order:] = twice
        eliminate(solve, unit, hooks)
        if order // PANEL in hooks:
            hooks[order // PANEL]()
        turns[step, square] = orthogonal(solve[:, order:])
        low_copy(step).start()

    def rotate_factor(step):
        turned = mix(turns[step, square], jnp.concatenate([stay_fac[...], held_fac[step]], axis=0))
        stay_fac[...] = turned[upper]
        sent_fac[step] = turned[lower]

    def meet(step):
        moving_copy(step).wait_recv()
        cross[step, row_place] = cross_of(near_moving[step], own(step))

    def share(step):
        for off in range(1, peers):
            cross_copy(step, off).start()

    def meet_first():
        meet(0)
        stay_copy().wait_recv()
        first[2, row_place] = cross_of(near_stay[0], own(0))

    def share_first():
        share(0)
        for off in range(1, peers):
            first_copy(2, off).start()

    last = STEPS - 1
    gram_copy(0).start()
    rotation(0, {MEET: meet_first, SHARE: share_first})
    top_copy(0).start()
    for off in range(1, peers):
        first_copy(2, off).wait_recv()
    turns[0, beyond] = peer_sum(first, 2)

    def advance(step, carry):
        then = step + 1
        top = turns[step, upper]
        top_wide = jnp.concatenate([top, jnp.zeros_like(top)], axis=0)
        grams[then, upper] = six_nt(six_nn(top, grams[step]), top_wide)
        stay[then] = mix(top, own(step))

        @pl.when(step > 0)
        def _():
            fac_copy(step - 1).wait_recv()

        rotate_factor(step)
        fac_copy(step).start()
        gram_copy(step).wait_recv()
        scale[...] = scale_of(trace(grams[step]) + trace(near_grams[step]))
        for off in range(1, peers):
            cross_copy(step, off).wait_recv()
        whole = jnp.concatenate([turns[step, beyond], peer_sum(cross, step)], axis=0)
        reach[...] = six_nt(whole, top_wide)
        reach_across[...] = six_nt(top, whole)
        low_copy(step).wait_recv()
        low = near_turns[step, lower]
        moving[then] = mix(low, near(step))
        moving_copy(then).start()
        low_wide = jnp.concatenate([jnp.zeros_like(low), low], axis=0)
        reach[...] += six_nt(near_grams[step], low_wide)
        grams[then, upper] += six_nt(reach_across[...], low_wide)
        grams[then, lower] = six_nn(low, reach[...])

        @pl.when(then < last)
        def _():
            gram_copy(then).start()

        def share_then():
            @pl.when(then < last)
            def _():
                share(then)

        rotation(then, {MEET: lambda: meet(then), SHARE: share_then})

        @pl.when(then < last)
        def _():
            top_copy(then).start()

        top_copy(step).wait_recv()
        arrived = near_turns[step, upper]
        near_stay[then] = mix(arrived, near(step))
        turns[then, beyond] = dot_nn(arrived, reach[...])
        return carry

    lax.fori_loop(0, last, advance, 0)
    fac_copy(last - 1).wait_recv()
    rotate_factor(last)
    fac_copy(last).start()
    new_columns[upper, :] = mix(turns[last, upper], own(last))
    new_factor[upper, :] = stay_fac[...]
    low_copy(last).wait_recv()
    new_columns[lower, :] = mix(near_turns[last, lower], near(last))
    fac_copy(last).wait_recv()
    new_factor[lower, :] = held_fac[STEPS]

    stay_copy().wait_send()
    for off in range(1, peers):
        for slot in range(3):
            first_copy(slot, off).wait_send()
    for step in range(STEPS):
        moving_copy(step).wait_send()
        fac_copy(step).wait_send()
        low_copy(step).wait_send()
        if step < last:
            gram_copy(step).wait_send()
            top_copy(step).wait_send()
            for off in range(1, peers):
                cross_copy(step, off).wait_send()


def body(columns, right_factor):
    order, width = columns.shape
    half = order // 2
    fac_width = right_factor.shape[1]
    peers = lax.axis_size("rows")

    def room(*shape):
        return pltpu.VMEM(shape, jnp.float32)

    def flags(*shape):
        return pltpu.SemaphoreType.DMA(shape)

    return pl.pallas_call(
        cycle_kernel,
        out_shape=[jax.ShapeDtypeStruct(a.shape, a.dtype) for a in (columns, right_factor)],
        in_specs=[pl.BlockSpec(memory_space=pltpu.VMEM)] * 2,
        out_specs=[pl.BlockSpec(memory_space=pltpu.VMEM)] * 2,
        scratch_shapes=[
            room(STEPS, half, width),
            room(STEPS, half, width),
            room(STEPS, half, width),
            room(STEPS, half, width),
            room(half, fac_width),
            room(STEPS, half, fac_width),
            room(STEPS + 1, half, fac_width),
            room(STEPS, order, order),
            room(STEPS, order, order),
            room(STEPS, order + half, order),
            room(STEPS, order, order),
            room(3, peers, half, order),
            room(STEPS, peers, half, order),
            room(order, order),
            room(half, order),
            room(8, LANES),
            room(8, LANES),
            room(order, 2 * order),
            pltpu.SemaphoreType.DMA,
            pltpu.SemaphoreType.DMA,
            flags(STEPS),
            flags(STEPS),
            flags(STEPS),
            flags(STEPS),
            flags(STEPS),
            flags(STEPS),
            flags(STEPS),
            flags(STEPS),
            flags(STEPS),
            flags(STEPS),
            flags(3, peers - 1),
            flags(3, peers - 1),
            flags(STEPS, peers - 1),
            flags(STEPS, peers - 1),
        ],
        compiler_params=pltpu.CompilerParams(
            collective_id=0, has_side_effects=True, vmem_limit_bytes=24 * 1024 * 1024
        ),
        name="cycle",
    )(columns, right_factor)


def solution(mesh):
    return jax.shard_map(
        body,
        mesh=mesh,
        in_specs=(P("blk", "rows"), P("blk", "rows")),
        out_specs=(P("blk", "rows"), P("blk", "rows")),
        check_vma=False,
    )
```

```python
import jax
import jax.numpy as jnp
from jax import lax
from jax.experimental import pallas as pl
from jax.experimental.pallas import tpu as pltpu
from jax.sharding import PartitionSpec as P

STEPS = 6
PANEL = 16
MEET = 5
SHARE = 6
LANES = 128
ROWS = 8
MESH = pl.DeviceIdType.MESH

HIGHEST_PREC = lax.Precision.HIGHEST


def dot_nn(a, b):
    return lax.dot_general(
        a, b, (((1,), (0,)), ((), ())), precision=HIGHEST_PREC, preferred_element_type=jnp.float32
    )


def dot_nt(a, b):
    return lax.dot_general(
        a, b, (((1,), (1,)), ((), ())), precision=HIGHEST_PREC, preferred_element_type=jnp.float32
    )


def dot_tn(a, b):
    return lax.dot_general(
        a, b, (((0,), (0,)), ((), ())), precision=HIGHEST_PREC, preferred_element_type=jnp.float32
    )


def split(a):
    high = a.astype(jnp.bfloat16)
    return high, (a - high.astype(jnp.float32)).astype(jnp.bfloat16)


def split_left(a, axis=1):
    high, low = split(a)
    return jnp.concatenate([high, low, high], axis=axis)


def split_right(b, axis=0):
    high, low = split(b)
    return jnp.concatenate([high, high, low], axis=axis)


def split_three(a):
    high = a.astype(jnp.bfloat16)
    rest = a - high.astype(jnp.float32)
    mid = rest.astype(jnp.bfloat16)
    return high, mid, (rest - mid.astype(jnp.float32)).astype(jnp.bfloat16)


def six_left(a):
    high, mid, low = split_three(a)
    return jnp.concatenate([low, high, mid, mid, high, high], axis=1)


def six_right(b, axis):
    high, mid, low = split_three(b)
    return jnp.concatenate([high, low, mid, high, mid, high], axis=axis)


def six_nn(a, b):
    return lax.dot_general(
        six_left(a), six_right(b, 0), (((1,), (0,)), ((), ())), preferred_element_type=jnp.float32
    )


def six_nt(a, b):
    return lax.dot_general(
        six_left(a), six_right(b, 1), (((1,), (1,)), ((), ())), preferred_element_type=jnp.float32
    )


def mix(turn, block):
    return lax.dot_general(
        split_left(turn), split_right(block), (((1,), (0,)), ((), ())), preferred_element_type=jnp.float32
    )


def cross_of(a, b):
    return lax.dot_general(
        split_left(a), split_right(b, 1), (((1,), (1,)), ((), ())), preferred_element_type=jnp.float32
    )


def spread_row(block, row):
    return jnp.broadcast_to(block[row : row + 1, :], block.shape)


def spread_lane(block, lane):
    return jnp.broadcast_to(block[:, lane : lane + 1], (block.shape[0], LANES))


def tree_sum(terms):
    while len(terms) > 1:
        terms = [sum(terms[i : i + 2][1:], terms[i]) for i in range(0, len(terms), 2)]
    return terms[0]


def eliminate(work, unit, hooks):
    order, width = work.shape
    panels = order // PANEL
    one = unit[...]
    wide_one = jnp.concatenate([one, one], axis=0)
    ahead = work[:PANEL, :]
    tiles = range(width // LANES)
    down = lax.broadcasted_iota(jnp.int32, (ROWS, LANES), 0)

    def part(block, group, t):
        return block[group * ROWS : (group + 1) * ROWS, t * LANES : (t + 1) * LANES]

    for panel in range(panels):
        if panel in hooks:
            hooks[panel]()
        low = panel * PANEL
        high = low + PANEL
        end = min(high + PANEL, order)
        own = ahead
        rows = [[part(own, g, t) for t in tiles] for g in range(2)]
        result = [rows[0][1], rows[1][1]]
        first_heads, second_heads = [], []
        for k in range(ROWS):
            both = spread_lane(own[:, :LANES], low + k) * wide_one
            first_heads.append(both[:ROWS])
            second_heads.append(both[ROWS:])
        for k in range(ROWS, PANEL):
            second_heads.append(spread_lane(rows[1][0], low + k) * one)
        scales = [jnp.zeros((ROWS, LANES), jnp.float32) for g in range(2)]
        pivot = spread_row(first_heads[0], 0)
        for j in range(ROWS):
            root = lax.rsqrt(pivot)
            inverse = root * root
            if j + 1 < ROWS:
                side = spread_row(first_heads[j], j + 1) * root
                pivot = spread_row(first_heads[j + 1], j + 1) - side * side
            else:
                side = spread_row(second_heads[j], 0) * root
                pivot = spread_row(second_heads[j + 1], 0) - side * side
            column = [first_heads[j] * inverse, second_heads[j] * inverse]
            onward = jnp.where(down > j, column[0], 0.0)
            column[0] = jnp.where(down == j, 1.0 - inverse, column[0])
            scales[0] = jnp.where(down == j, root, scales[0])
            front = [spread_row(rows[0][t], j) for t in tiles]
            rows = [[rows[g][t] - column[g] * front[t] for t in tiles] for g in range(2)]
            front = spread_row(result[0], j)
            result = [result[0] - onward * front, result[1] - column[1] * front]
            for k in range(j + 1, ROWS):
                head = spread_row(first_heads[k], j)
                first_heads[k] = first_heads[k] - column[0] * head
                second_heads[k] = second_heads[k] - column[1] * head
            for k in range(ROWS, PANEL):
                head = spread_row(second_heads[j], k - ROWS)
                second_heads[k] = second_heads[k] - column[1] * head
        above = [spread_lane(rows[0][0], low + k) for k in range(ROWS, PANEL)]
        for j in range(ROWS, PANEL):
            row = j - ROWS
            root = lax.rsqrt(pivot)
            inverse = root * root
            if j + 1 < PANEL:
                side = spread_row(second_heads[j], row + 1) * root
                pivot = spread_row(second_heads[j + 1], row + 1) - side * side
            column = second_heads[j] * inverse
            onward = jnp.where(down > row, column, 0.0)
            column = jnp.where(down == row, 1.0 - inverse, column)
            scales[1] = jnp.where(down == row, root, scales[1])
            rows[1] = [rows[1][t] - column * spread_row(rows[1][t], row) for t in tiles]
            result[1] = result[1] - onward * spread_row(result[1], row)
            for k in range(j + 1, PANEL):
                second_heads[k] = second_heads[k] - column * spread_row(second_heads[k], row)
        for g in range(2):
            start = low + g * ROWS
            work[start : start + ROWS, LANES:] = result[g] * scales[g]
        if end == high:
            continue
        fronts = [[spread_row(rows[1][t], k) for t in tiles] for k in range(ROWS)]
        rows[0] = [
            rows[0][t] - tree_sum([above[k] * fronts[k][t] for k in range(ROWS)]) for t in tiles
        ]
        fronts = [[spread_row(rows[0][t], k) for t in tiles] for k in range(ROWS)] + fronts
        below = work[high:end, :]
        heads = [spread_lane(below[:, :LANES], low + k) for k in range(PANEL)]
        ahead = []
        for g in range(2):
            moved = [
                tree_sum([part(heads[k], g, 0) * fronts[k][t] for k in range(PANEL)]) for t in tiles
            ]
            ahead.append(jnp.concatenate([part(below, g, t) - moved[t] for t in tiles], axis=1))
        ahead = jnp.concatenate(ahead, axis=0)
        if end < order:
            solved = jnp.concatenate([jnp.concatenate(rows[g], axis=1) for g in range(2)], axis=0)
            work[end:, :] = work[end:, :] - trailing(work, low, high, end, solved)


def trailing(work, low, high, end, solved):
    order = work.shape[0]
    parts = [jnp.zeros((low, solved.shape[1]), jnp.float32)] if low else []
    parts += [solved, jnp.zeros((order - high, solved.shape[1]), jnp.float32)]
    return dot_nn(work[end:, :order], jnp.concatenate(parts, axis=0))


def grid_of(shape):
    return lax.broadcasted_iota(jnp.int32, shape, 0), lax.broadcasted_iota(jnp.int32, shape, 1)


def trace(square):
    down, across = grid_of(square.shape)
    kept = jnp.where(down == across, square, 0.0)
    return jnp.sum(jnp.sum(kept, axis=0, keepdims=True), axis=1, keepdims=True)


def scale_of(total):
    return jnp.broadcast_to(1.0 / (total * total), (8, LANES))


def orthogonal(turn):
    overlap = six_nt(turn, turn)
    down, across = grid_of(overlap.shape)
    lower = jnp.where(down > across, overlap, 0.0)
    lower = jnp.where(down == across, 0.5 * (overlap - 1.0), lower)
    return turn - mix(lower, turn)


def cycle_kernel(
    columns, right_factor, new_columns, new_factor, stay, moving, near_stay, near_moving, stay_fac, sent_fac,
    held_fac, grams, near_grams, turns, near_turns, first, cross, reach, reach_across, scale, unit, solve, stay_sent,
    stay_sem, moving_sent, moving_sem, fac_sent, fac_sem, gram_sent, gram_sem, low_sent, low_sem, top_sent,
    top_sem, first_sent, first_sem, cross_sent, cross_sem,
):
    half = columns.shape[0] // 2
    order = 2 * half
    upper, lower, beyond = slice(0, half), slice(half, order), slice(order, order + half)
    square = slice(0, order)
    ring, peers = lax.axis_size("blk"), lax.axis_size("rows")
    place, row_place = lax.axis_index("blk"), lax.axis_index("rows")
    right, left = lax.rem(place + 1, ring), lax.rem(place + ring - 1, ring)

    barrier = pltpu.get_barrier_semaphore()
    for neighbour in (left, right):
        pl.semaphore_signal(barrier, inc=1, device_id={"blk": neighbour}, device_id_type=MESH)
    for off in range(1, peers):
        peer = lax.rem(row_place + off, peers)
        pl.semaphore_signal(barrier, inc=1, device_id={"rows": peer}, device_id_type=MESH)

    def to_right(source, target, send_sem, recv_sem):
        return pltpu.make_async_remote_copy(
            src_ref=source,
            dst_ref=target,
            send_sem=send_sem,
            recv_sem=recv_sem,
            device_id={"blk": right},
            device_id_type=MESH,
        )

    def stay_copy():
        return to_right(stay.at[0], near_stay.at[0], stay_sent, stay_sem)

    def moving_copy(step):
        return to_right(
            moving.at[step], near_moving.at[step], moving_sent.at[step], moving_sem.at[step]
        )

    def fac_copy(step):
        return to_right(
            sent_fac.at[step], held_fac.at[step + 1], fac_sent.at[step], fac_sem.at[step]
        )

    def gram_copy(step):
        return to_right(
            grams.at[step], near_grams.at[step], gram_sent.at[step], gram_sem.at[step]
        )

    def low_copy(step):
        return to_right(
            turns.at[step, lower], near_turns.at[step, lower], low_sent.at[step], low_sem.at[step]
        )

    def top_copy(step):
        return to_right(
            turns.at[step, upper], near_turns.at[step, upper], top_sent.at[step], top_sem.at[step]
        )

    def to_peer(part, send_sem, recv_sem, off):
        return pltpu.make_async_remote_copy(
            src_ref=part,
            dst_ref=part,
            send_sem=send_sem.at[off - 1],
            recv_sem=recv_sem.at[off - 1],
            device_id={"rows": lax.rem(row_place + off, peers)},
            device_id_type=MESH,
        )

    def first_copy(slot, off):
        return to_peer(first.at[slot, row_place], first_sent.at[slot], first_sem.at[slot], off)

    def cross_copy(step, off):
        return to_peer(cross.at[step, row_place], cross_sent.at[step], cross_sem.at[step], off)

    def peer_sum(parts, slot):
        total = parts[slot, 0]
        for peer in range(1, peers):
            total = total + parts[slot, peer]
        return total

    def own(step):
        return jnp.concatenate([stay[step], moving[step]], axis=0)

    def near(step):
        return jnp.concatenate([near_stay[step], near_moving[step]], axis=0)

    unit[...] = jnp.ones_like(unit)
    stay[0] = columns[upper, :]
    moving[0] = columns[lower, :]
    stay_fac[...] = right_factor[upper, :]
    held_fac[0] = right_factor[lower, :]
    pl.semaphore_wait(barrier, 2 + peers - 1)
    moving_copy(0).start()
    stay_copy().start()
    pair = columns[...]
    start = cross_of(pair, pair)
    first[0, row_place] = start[upper]
    first[1, row_place] = start[lower]
    for off in range(1, peers):
        for slot in range(2):
            first_copy(slot, off).start()
    for off in range(1, peers):
        for slot in range(2):
            first_copy(slot, off).wait_recv()
    grams[0, upper] = peer_sum(first, 0)
    grams[0, lower] = peer_sum(first, 1)
    scale[...] = scale_of(trace(grams[0]))

    def rotation(step, hooks):
        gram = grams[step]
        twice = six_nn(gram, gram) * scale[:1, :]
        solve[:, :order] = six_nn(twice, twice)
        solve[:, order:] = twice
        eliminate(solve, unit, hooks)
        if order // PANEL in hooks:
            hooks[order // PANEL]()
        turns[step, square] = orthogonal(solve[:, order:])
        low_copy(step).start()

    def rotate_factor(step):
        turned = mix(turns[step, square], jnp.concatenate([stay_fac[...], held_fac[step]], axis=0))
        stay_fac[...] = turned[upper]
        sent_fac[step] = turned[lower]

    def meet(step):
        moving_copy(step).wait_recv()
        cross[step, row_place] = cross_of(near_moving[step], own(step))

    def share(step):
        for off in range(1, peers):
            cross_copy(step, off).start()

    def meet_first():
        meet(0)
        stay_copy().wait_recv()
        first[2, row_place] = cross_of(near_stay[0], own(0))

    def share_first():
        share(0)
        for off in range(1, peers):
            first_copy(2, off).start()

    last = STEPS - 1
    gram_copy(0).start()
    rotation(0, {MEET: meet_first, SHARE: share_first})
    top_copy(0).start()
    rotate_factor(0)
    fac_copy(0).start()
    for off in range(1, peers):
        first_copy(2, off).wait_recv()
    turns[0, beyond] = peer_sum(first, 2)

    def advance(step, carry):
        then = step + 1
        top = turns[step, upper]
        top_wide = jnp.concatenate([top, jnp.zeros_like(top)], axis=0)
        grams[then, upper] = six_nt(six_nn(top, grams[step]), top_wide)
        stay[then] = mix(top, own(step))

        gram_copy(step).wait_recv()
        scale[...] = scale_of(trace(grams[step]) + trace(near_grams[step]))
        for off in range(1, peers):
            cross_copy(step, off).wait_recv()
        whole = jnp.concatenate([turns[step, beyond], peer_sum(cross, step)], axis=0)
        reach[...] = six_nt(whole, top_wide)
        reach_across[...] = six_nt(top, whole)
        low_copy(step).wait_recv()
        low = near_turns[step, lower]
        moving[then] = mix(low, near(step))
        moving_copy(then).start()
        low_wide = jnp.concatenate([jnp.zeros_like(low), low], axis=0)
        reach[...] += six_nt(near_grams[step], low_wide)
        grams[then, upper] += six_nt(reach_across[...], low_wide)
        grams[then, lower] = six_nn(low, reach[...])

        @pl.when(then < last)
        def _():
            gram_copy(then).start()

        def share_then():
            @pl.when(then < last)
            def _():
                share(then)

        rotation(then, {MEET: lambda: meet(then), SHARE: share_then})

        @pl.when(then < last)
        def _():
            top_copy(then).start()

        fac_copy(step).wait_recv()
        rotate_factor(then)
        fac_copy(then).start()
        top_copy(step).wait_recv()
        arrived = near_turns[step, upper]
        near_stay[then] = mix(arrived, near(step))
        turns[then, beyond] = dot_nn(arrived, reach[...])
        return carry

    lax.fori_loop(0, last, advance, 0)
    new_columns[upper, :] = mix(turns[last, upper], own(last))
    new_factor[upper, :] = stay_fac[...]
    low_copy(last).wait_recv()
    new_columns[lower, :] = mix(near_turns[last, lower], near(last))
    fac_copy(last).wait_recv()
    new_factor[lower, :] = held_fac[STEPS]

    stay_copy().wait_send()
    for off in range(1, peers):
        for slot in range(3):
            first_copy(slot, off).wait_send()
    for step in range(STEPS):
        moving_copy(step).wait_send()
        fac_copy(step).wait_send()
        low_copy(step).wait_send()
        if step < last:
            gram_copy(step).wait_send()
            top_copy(step).wait_send()
            for off in range(1, peers):
                cross_copy(step, off).wait_send()


def body(columns, right_factor):
    order, width = columns.shape
    half = order // 2
    fac_width = right_factor.shape[1]
    peers = lax.axis_size("rows")

    def room(*shape):
        return pltpu.VMEM(shape, jnp.float32)

    def flags(*shape):
        return pltpu.SemaphoreType.DMA(shape)

    return pl.pallas_call(
        cycle_kernel,
        out_shape=[jax.ShapeDtypeStruct(a.shape, a.dtype) for a in (columns, right_factor)],
        in_specs=[pl.BlockSpec(memory_space=pltpu.VMEM)] * 2,
        out_specs=[pl.BlockSpec(memory_space=pltpu.VMEM)] * 2,
        scratch_shapes=[
            room(STEPS, half, width),
            room(STEPS, half, width),
            room(STEPS, half, width),
            room(STEPS, half, width),
            room(half, fac_width),
            room(STEPS, half, fac_width),
            room(STEPS + 1, half, fac_width),
            room(STEPS, order, order),
            room(STEPS, order, order),
            room(STEPS, order + half, order),
            room(STEPS, order, order),
            room(3, peers, half, order),
            room(STEPS, peers, half, order),
            room(order, order),
            room(half, order),
            room(8, LANES),
            room(8, LANES),
            room(order, 2 * order),
            pltpu.SemaphoreType.DMA,
            pltpu.SemaphoreType.DMA,
            flags(STEPS),
            flags(STEPS),
            flags(STEPS),
            flags(STEPS),
            flags(STEPS),
            flags(STEPS),
            flags(STEPS),
            flags(STEPS),
            flags(STEPS),
            flags(STEPS),
            flags(3, peers - 1),
            flags(3, peers - 1),
            flags(STEPS, peers - 1),
            flags(STEPS, peers - 1),
        ],
        compiler_params=pltpu.CompilerParams(
            collective_id=0, has_side_effects=True, vmem_limit_bytes=24 * 1024 * 1024
        ),
        name="cycle",
    )(columns, right_factor)


def solution(mesh):
    return jax.shard_map(
        body,
        mesh=mesh,
        in_specs=(P("blk", "rows"), P("blk", "rows")),
        out_specs=(P("blk", "rows"), P("blk", "rows")),
        check_vma=False,
    )
```

```python
import jax
import jax.numpy as jnp
from jax import lax
from jax.experimental import pallas as pl
from jax.experimental.pallas import tpu as pltpu
from jax.sharding import PartitionSpec as P

STEPS = 6
PANEL = 16
MEET = 5
SHARE = 6
LANES = 128
ROWS = 8
MESH = pl.DeviceIdType.MESH

HIGHEST_PREC = lax.Precision.HIGHEST


def dot_nn(a, b):
    return lax.dot_general(
        a, b, (((1,), (0,)), ((), ())), precision=HIGHEST_PREC, preferred_element_type=jnp.float32
    )


def dot_nt(a, b):
    return lax.dot_general(
        a, b, (((1,), (1,)), ((), ())), precision=HIGHEST_PREC, preferred_element_type=jnp.float32
    )


def dot_tn(a, b):
    return lax.dot_general(
        a, b, (((0,), (0,)), ((), ())), precision=HIGHEST_PREC, preferred_element_type=jnp.float32
    )


def split(a):
    high = a.astype(jnp.bfloat16)
    return high, (a - high.astype(jnp.float32)).astype(jnp.bfloat16)


def split_left(a, axis=1):
    high, low = split(a)
    return jnp.concatenate([high, low, high], axis=axis)


def split_right(b, axis=0):
    high, low = split(b)
    return jnp.concatenate([high, high, low], axis=axis)


def split_three(a):
    high = a.astype(jnp.bfloat16)
    rest = a - high.astype(jnp.float32)
    mid = rest.astype(jnp.bfloat16)
    return high, mid, (rest - mid.astype(jnp.float32)).astype(jnp.bfloat16)


def six_left(a):
    high, mid, low = split_three(a)
    return jnp.concatenate([low, high, mid, mid, high, high], axis=1)


def six_right(b, axis):
    high, mid, low = split_three(b)
    return jnp.concatenate([high, low, mid, high, mid, high], axis=axis)


def six_nn(a, b):
    return lax.dot_general(
        six_left(a), six_right(b, 0), (((1,), (0,)), ((), ())), preferred_element_type=jnp.float32
    )


def six_nt(a, b):
    return lax.dot_general(
        six_left(a), six_right(b, 1), (((1,), (1,)), ((), ())), preferred_element_type=jnp.float32
    )


def mix(turn, block):
    return lax.dot_general(
        split_left(turn), split_right(block), (((1,), (0,)), ((), ())), preferred_element_type=jnp.float32
    )


def cross_of(a, b):
    return lax.dot_general(
        split_left(a), split_right(b, 1), (((1,), (1,)), ((), ())), preferred_element_type=jnp.float32
    )


def spread_row(block, row):
    return jnp.broadcast_to(block[row : row + 1, :], block.shape)


def spread_lane(block, lane):
    return jnp.broadcast_to(block[:, lane : lane + 1], (block.shape[0], LANES))


def tree_sum(terms):
    while len(terms) > 1:
        terms = [sum(terms[i : i + 2][1:], terms[i]) for i in range(0, len(terms), 2)]
    return terms[0]


def eliminate(work, unit, hooks):
    order, width = work.shape
    panels = order // PANEL
    one = unit[...]
    wide_one = jnp.concatenate([one, one], axis=0)
    ahead = work[:PANEL, :]
    tiles = range(width // LANES)
    down = lax.broadcasted_iota(jnp.int32, (ROWS, LANES), 0)

    def part(block, group, t):
        return block[group * ROWS : (group + 1) * ROWS, t * LANES : (t + 1) * LANES]

    for panel in range(panels):
        if panel in hooks:
            hooks[panel]()
        low = panel * PANEL
        high = low + PANEL
        end = min(high + PANEL, order)
        own = ahead
        rows = [[part(own, g, t) for t in tiles] for g in range(2)]
        result = [rows[0][1], rows[1][1]]
        first_heads, second_heads = [], []
        for k in range(ROWS):
            both = spread_lane(own[:, :LANES], low + k) * wide_one
            first_heads.append(both[:ROWS])
            second_heads.append(both[ROWS:])
        for k in range(ROWS, PANEL):
            second_heads.append(spread_lane(rows[1][0], low + k) * one)
        scales = [jnp.zeros((ROWS, LANES), jnp.float32) for g in range(2)]
        pivot = spread_row(first_heads[0], 0)
        for j in range(ROWS):
            root = lax.rsqrt(pivot)
            inverse = root * root
            if j + 1 < ROWS:
                side = spread_row(first_heads[j], j + 1) * root
                pivot = spread_row(first_heads[j + 1], j + 1) - side * side
            else:
                side = spread_row(second_heads[j], 0) * root
                pivot = spread_row(second_heads[j + 1], 0) - side * side
            column = [first_heads[j] * inverse, second_heads[j] * inverse]
            onward = jnp.where(down > j, column[0], 0.0)
            column[0] = jnp.where(down == j, 1.0 - inverse, column[0])
            scales[0] = jnp.where(down == j, root, scales[0])
            front = [spread_row(rows[0][t], j) for t in tiles]
            rows = [[rows[g][t] - column[g] * front[t] for t in tiles] for g in range(2)]
            front = spread_row(result[0], j)
            result = [result[0] - onward * front, result[1] - column[1] * front]
            for k in range(j + 1, ROWS):
                head = spread_row(first_heads[k], j)
                first_heads[k] = first_heads[k] - column[0] * head
                second_heads[k] = second_heads[k] - column[1] * head
            for k in range(ROWS, PANEL):
                head = spread_row(second_heads[j], k - ROWS)
                second_heads[k] = second_heads[k] - column[1] * head
        above = [spread_lane(rows[0][0], low + k) for k in range(ROWS, PANEL)]
        for j in range(ROWS, PANEL):
            row = j - ROWS
            root = lax.rsqrt(pivot)
            inverse = root * root
            if j + 1 < PANEL:
                side = spread_row(second_heads[j], row + 1) * root
                pivot = spread_row(second_heads[j + 1], row + 1) - side * side
            column = second_heads[j] * inverse
            onward = jnp.where(down > row, column, 0.0)
            column = jnp.where(down == row, 1.0 - inverse, column)
            scales[1] = jnp.where(down == row, root, scales[1])
            rows[1] = [rows[1][t] - column * spread_row(rows[1][t], row) for t in tiles]
            result[1] = result[1] - onward * spread_row(result[1], row)
            for k in range(j + 1, PANEL):
                second_heads[k] = second_heads[k] - column * spread_row(second_heads[k], row)
        for g in range(2):
            start = low + g * ROWS
            work[start : start + ROWS, LANES:] = result[g] * scales[g]
        if end == high:
            continue
        fronts = [[spread_row(rows[1][t], k) for t in tiles] for k in range(ROWS)]
        rows[0] = [
            rows[0][t] - tree_sum([above[k] * fronts[k][t] for k in range(ROWS)]) for t in tiles
        ]
        fronts = [[spread_row(rows[0][t], k) for t in tiles] for k in range(ROWS)] + fronts
        below = work[high:end, :]
        heads = [spread_lane(below[:, :LANES], low + k) for k in range(PANEL)]
        ahead = []
        for g in range(2):
            moved = [
                tree_sum([part(heads[k], g, 0) * fronts[k][t] for k in range(PANEL)]) for t in tiles
            ]
            ahead.append(jnp.concatenate([part(below, g, t) - moved[t] for t in tiles], axis=1))
        ahead = jnp.concatenate(ahead, axis=0)
        if end < order:
            solved = jnp.concatenate([jnp.concatenate(rows[g], axis=1) for g in range(2)], axis=0)
            work[end:, :] = work[end:, :] - trailing(work, low, high, end, solved)


def trailing(work, low, high, end, solved):
    order = work.shape[0]
    parts = [jnp.zeros((low, solved.shape[1]), jnp.float32)] if low else []
    parts += [solved, jnp.zeros((order - high, solved.shape[1]), jnp.float32)]
    return dot_nn(work[end:, :order], jnp.concatenate(parts, axis=0))


def grid_of(shape):
    return lax.broadcasted_iota(jnp.int32, shape, 0), lax.broadcasted_iota(jnp.int32, shape, 1)


def trace(square):
    down, across = grid_of(square.shape)
    kept = jnp.where(down == across, square, 0.0)
    return jnp.sum(jnp.sum(kept, axis=0, keepdims=True), axis=1, keepdims=True)


def scale_of(total):
    return jnp.broadcast_to(1.0 / (total * total), (8, LANES))


def orthogonal(turn):
    overlap = six_nt(turn, turn)
    down, across = grid_of(overlap.shape)
    lower = jnp.where(down > across, overlap, 0.0)
    lower = jnp.where(down == across, 0.5 * (overlap - 1.0), lower)
    return turn - mix(lower, turn)


def cycle_kernel(
    columns, right_factor, new_columns, new_factor, stay, moving, near_stay, near_moving, stay_fac, sent_fac,
    held_fac, grams, near_grams, turns, near_turns, first, cross, reach, reach_across, scale, unit, solve, stay_sent,
    stay_sem, moving_sent, moving_sem, fac_sent, fac_sem, gram_sent, gram_sem, low_sent, low_sem, top_sent,
    top_sem, first_sent, first_sem, cross_sent, cross_sem,
):
    half = columns.shape[0] // 2
    order = 2 * half
    upper, lower, beyond = slice(0, half), slice(half, order), slice(order, order + half)
    square = slice(0, order)
    ring, peers = lax.axis_size("blk"), lax.axis_size("rows")
    place, row_place = lax.axis_index("blk"), lax.axis_index("rows")
    right, left = lax.rem(place + 1, ring), lax.rem(place + ring - 1, ring)

    barrier = pltpu.get_barrier_semaphore()
    for neighbour in (left, right):
        pl.semaphore_signal(barrier, inc=1, device_id={"blk": neighbour}, device_id_type=MESH)
    for off in range(1, peers):
        peer = lax.rem(row_place + off, peers)
        pl.semaphore_signal(barrier, inc=1, device_id={"rows": peer}, device_id_type=MESH)

    def to_right(source, target, send_sem, recv_sem):
        return pltpu.make_async_remote_copy(
            src_ref=source,
            dst_ref=target,
            send_sem=send_sem,
            recv_sem=recv_sem,
            device_id={"blk": right},
            device_id_type=MESH,
        )

    def stay_copy():
        return to_right(stay.at[0], near_stay.at[0], stay_sent, stay_sem)

    def moving_copy(step):
        return to_right(
            moving.at[step], near_moving.at[step], moving_sent.at[step], moving_sem.at[step]
        )

    def fac_copy(step):
        return to_right(
            sent_fac.at[step], held_fac.at[step + 1], fac_sent.at[step], fac_sem.at[step]
        )

    def gram_copy(step):
        return to_right(
            grams.at[step], near_grams.at[step], gram_sent.at[step], gram_sem.at[step]
        )

    def low_copy(step):
        return to_right(
            turns.at[step, lower], near_turns.at[step, lower], low_sent.at[step], low_sem.at[step]
        )

    def top_copy(step):
        return to_right(
            turns.at[step, upper], near_turns.at[step, upper], top_sent.at[step], top_sem.at[step]
        )

    def to_peer(part, send_sem, recv_sem, off):
        return pltpu.make_async_remote_copy(
            src_ref=part,
            dst_ref=part,
            send_sem=send_sem.at[off - 1],
            recv_sem=recv_sem.at[off - 1],
            device_id={"rows": lax.rem(row_place + off, peers)},
            device_id_type=MESH,
        )

    def first_copy(slot, off):
        return to_peer(first.at[slot, row_place], first_sent.at[slot], first_sem.at[slot], off)

    def cross_copy(step, off):
        return to_peer(cross.at[step, row_place], cross_sent.at[step], cross_sem.at[step], off)

    def peer_sum(parts, slot):
        total = parts[slot, 0]
        for peer in range(1, peers):
            total = total + parts[slot, peer]
        return total

    def own(step):
        return jnp.concatenate([stay[step], moving[step]], axis=0)

    def near(step):
        return jnp.concatenate([near_stay[step], near_moving[step]], axis=0)

    unit[...] = jnp.ones_like(unit)
    stay[0] = columns[upper, :]
    moving[0] = columns[lower, :]
    stay_fac[...] = right_factor[upper, :]
    held_fac[0] = right_factor[lower, :]
    pl.semaphore_wait(barrier, 2 + peers - 1)
    moving_copy(0).start()
    stay_copy().start()
    pair = columns[...]
    start = cross_of(pair, pair)
    first[0, row_place] = start[upper]
    first[1, row_place] = start[lower]
    for off in range(1, peers):
        for slot in range(2):
            first_copy(slot, off).start()
    for off in range(1, peers):
        for slot in range(2):
            first_copy(slot, off).wait_recv()
    grams[0, upper] = peer_sum(first, 0)
    grams[0, lower] = peer_sum(first, 1)
    scale[...] = scale_of(trace(grams[0]))

    def rotation(step, hooks):
        gram = grams[step]
        twice = six_nn(gram, gram) * scale[:1, :]
        solve[:, :order] = six_nn(twice, twice)
        solve[:, order:] = twice
        eliminate(solve, unit, hooks)
        if order // PANEL in hooks:
            hooks[order // PANEL]()
        turns[step, square] = orthogonal(solve[:, order:])
        low_copy(step).start()

    def rotate_factor(step):
        turned = mix(turns[step, square], jnp.concatenate([stay_fac[...], held_fac[step]], axis=0))
        stay_fac[...] = turned[upper]
        sent_fac[step] = turned[lower]

    def meet(step):
        moving_copy(step).wait_recv()
        cross[step, row_place] = cross_of(near_moving[step], own(step))

    def share(step):
        for off in range(1, peers):
            cross_copy(step, off).start()

    def meet_first():
        meet(0)
        stay_copy().wait_recv()
        first[2, row_place] = cross_of(near_stay[0], own(0))

    def share_first():
        share(0)
        for off in range(1, peers):
            first_copy(2, off).start()

    last = STEPS - 1
    gram_copy(0).start()
    rotation(0, {MEET: meet_first, SHARE: share_first})
    top_copy(0).start()
    rotate_factor(0)
    fac_copy(0).start()
    for off in range(1, peers):
        first_copy(2, off).wait_recv()
    turns[0, beyond] = peer_sum(first, 2)

    def advance(step, carry):
        then = step + 1
        top = turns[step, upper]
        top_wide = jnp.concatenate([top, jnp.zeros_like(top)], axis=0)
        grams[then, upper] = six_nt(six_nn(top, grams[step]), top_wide)
        stay[then] = mix(top, own(step))

        gram_copy(step).wait_recv()
        scale[...] = scale_of(trace(grams[step]) + trace(near_grams[step]))
        for off in range(1, peers):
            cross_copy(step, off).wait_recv()
        whole = jnp.concatenate([turns[step, beyond], peer_sum(cross, step)], axis=0)
        reach[...] = six_nt(whole, top_wide)
        reach_across[...] = six_nt(top, whole)
        low_copy(step).wait_recv()
        low = near_turns[step, lower]
        moving[then] = mix(low, near(step))
        moving_copy(then).start()
        low_wide = jnp.concatenate([jnp.zeros_like(low), low], axis=0)
        reach[...] += six_nt(near_grams[step], low_wide)
        grams[then, upper] += six_nt(reach_across[...], low_wide)
        grams[then, lower] = six_nn(low, reach[...])

        @pl.when(then < last)
        def _():
            gram_copy(then).start()

        def share_then():
            @pl.when(then < last)
            def _():
                share(then)

        rotation(then, {MEET: lambda: meet(then), SHARE: share_then})

        @pl.when(then < last)
        def _():
            top_copy(then).start()

        fac_copy(step).wait_recv()
        rotate_factor(then)
        fac_copy(then).start()
        top_copy(step).wait_recv()
        arrived = near_turns[step, upper]
        near_stay[then] = mix(arrived, near(step))
        turns[then, beyond] = six_nn(arrived, reach[...])
        return carry

    lax.fori_loop(0, last, advance, 0)
    new_columns[upper, :] = mix(turns[last, upper], own(last))
    new_factor[upper, :] = stay_fac[...]
    low_copy(last).wait_recv()
    new_columns[lower, :] = mix(near_turns[last, lower], near(last))
    fac_copy(last).wait_recv()
    new_factor[lower, :] = held_fac[STEPS]

    stay_copy().wait_send()
    for off in range(1, peers):
        for slot in range(3):
            first_copy(slot, off).wait_send()
    for step in range(STEPS):
        moving_copy(step).wait_send()
        fac_copy(step).wait_send()
        low_copy(step).wait_send()
        if step < last:
            gram_copy(step).wait_send()
            top_copy(step).wait_send()
            for off in range(1, peers):
                cross_copy(step, off).wait_send()


def body(columns, right_factor):
    order, width = columns.shape
    half = order // 2
    fac_width = right_factor.shape[1]
    peers = lax.axis_size("rows")

    def room(*shape):
        return pltpu.VMEM(shape, jnp.float32)

    def flags(*shape):
        return pltpu.SemaphoreType.DMA(shape)

    return pl.pallas_call(
        cycle_kernel,
        out_shape=[jax.ShapeDtypeStruct(a.shape, a.dtype) for a in (columns, right_factor)],
        in_specs=[pl.BlockSpec(memory_space=pltpu.VMEM)] * 2,
        out_specs=[pl.BlockSpec(memory_space=pltpu.VMEM)] * 2,
        scratch_shapes=[
            room(STEPS, half, width),
            room(STEPS, half, width),
            room(STEPS, half, width),
            room(STEPS, half, width),
            room(half, fac_width),
            room(STEPS, half, fac_width),
            room(STEPS + 1, half, fac_width),
            room(STEPS, order, order),
            room(STEPS, order, order),
            room(STEPS, order + half, order),
            room(STEPS, order, order),
            room(3, peers, half, order),
            room(STEPS, peers, half, order),
            room(order, order),
            room(half, order),
            room(8, LANES),
            room(8, LANES),
            room(order, 2 * order),
            pltpu.SemaphoreType.DMA,
            pltpu.SemaphoreType.DMA,
            flags(STEPS),
            flags(STEPS),
            flags(STEPS),
            flags(STEPS),
            flags(STEPS),
            flags(STEPS),
            flags(STEPS),
            flags(STEPS),
            flags(STEPS),
            flags(STEPS),
            flags(3, peers - 1),
            flags(3, peers - 1),
            flags(STEPS, peers - 1),
            flags(STEPS, peers - 1),
        ],
        compiler_params=pltpu.CompilerParams(
            collective_id=0, has_side_effects=True, vmem_limit_bytes=24 * 1024 * 1024
        ),
        name="cycle",
    )(columns, right_factor)


def solution(mesh):
    return jax.shard_map(
        body,
        mesh=mesh,
        in_specs=(P("blk", "rows"), P("blk", "rows")),
        out_specs=(P("blk", "rows"), P("blk", "rows")),
        check_vma=False,
    )
```
